256 devices in a mesh: dp: 16 (over x, z_hi, core), expert: 16 (over y, z_lo).
Axes of the slice: x: 4, y: 4, z: 8 (z_hi: 2, z_lo: 4; z = z_hi * 4 + z_lo), core: 2. Of those that a mesh axis runs over, the one named last changes fastest.
Arguments:
- hidden: bfloat16 [16, 2048, 1792], P('expert', 'dp'), may hold values from -6 to 6
- outgrad: bfloat16 [16, 2048, 4096], P('expert', 'dp'), may hold values from -6 to 6
- row_expert: int32 [16, 2048], P('expert', 'dp'), may hold values from 0 to 1
- counts: int32 [16, 16], P('expert', 'dp'), may hold values from 1 to 128, as said below
- learner_map: int32 [256], replicated, may hold values from 0 to 255, as said below
- rollout_map: int32 [256], replicated, may hold values from 0 to 255, as said below
- master: float32 [4096, 28672], P('dp', 'expert'), may hold values from -3 to 3
- moment1: float32 [4096, 28672], P('dp', 'expert'), may hold values from -12 to 12
- moment2: float32 [4096, 28672], P('dp', 'expert'), may hold values from 1 to 1000
Outputs:
- new_master: float32 [4096, 28672], P('dp', 'expert')
- new_moment1: float32 [4096, 28672], P('dp', 'expert')
- new_moment2: float32 [4096, 28672], P('dp', 'expert')
- rollout_weights: bfloat16 [4096, 28672], P('dp', 'expert')
The draws below stay inside these ranges and needn't reach their ends.
Inputs may be any that keep to these rules, and one draw needn't show every extreme that they name: `counts`: some device has exactly 128 live rows in every draw. `learner_map`: a permutation of the units. `rollout_map`: a permutation of the units; the 16 units at the positions of one learner device lie at positions of 16 different rollout devices, one each.
All inputs are finite; a program needn't handle non-finite values.
Results may differ from the reference program's by a relative error of at most 0.0095.
Values may be sent and summed in bfloat16 or wider, within the bound.
A program may use at most 128 MiB of HBM per device.

```python
import math
import jax
import jax.numpy as jnp
from jax import lax

D = 4096
FF = 14336
EXP_WIN = 2
ROWS = 128
TOKROWS = 2048
UNITS = 256
BLOCK = 112
FF_DEV = 1792
N_DP = 16
N_EXPERT = 16


def draw_counts(key, part):
    first, second, third = jax.random.split(key, 3)
    shape = (N_EXPERT, N_DP)
    level = jax.random.randint(first, shape, 0, 4)
    base = ROWS // jnp.left_shift(jnp.ones(shape, jnp.int32), level)
    reduction = jax.random.randint(second, shape, 0, base // 2 + 1)
    values = base - reduction
    chosen = jax.random.randint(third, (), 0, N_EXPERT * N_DP)
    flat_index = jnp.arange(N_EXPERT * N_DP, dtype=jnp.int32).reshape(shape)
    return jnp.where(flat_index == chosen, ROWS, values).astype(jnp.int32)


def draw_both_maps(key):
    groups = N_EXPERT
    total = groups * groups
    learner = jax.random.permutation(jax.random.fold_in(key, 11), total).astype(jnp.int32)
    dest_keys = jax.random.split(jax.random.fold_in(key, 23), groups)
    destination = jax.vmap(lambda one: jax.random.permutation(one, groups))(dest_keys).astype(jnp.int32)
    slot_keys = jax.random.split(jax.random.fold_in(key, 37), groups)
    arrival = jax.vmap(lambda one: jax.random.permutation(one, groups))(slot_keys).astype(jnp.int32)
    source = jnp.broadcast_to(jnp.arange(groups, dtype=jnp.int32)[:, None], (groups, groups))
    position = destination * groups + arrival[destination, source]
    rollout = jnp.zeros((total,), jnp.int32).at[position.reshape(-1)].set(learner)
    return (learner, rollout)


def draw_learner_map(key, part):
    return draw_both_maps(key)[0]


def draw_rollout_map(key, part):
    return draw_both_maps(key)[1]


def place_ends(values, own_key, least, top_value):
    place = [jax.random.randint(jax.random.fold_in(own_key, axis), (), 0, length) for axis, length in enumerate(values.shape)]
    main_axis = values.shape.index(max(values.shape))
    beside = place[:main_axis] + [(place[main_axis] + 1) % values.shape[main_axis]] + place[main_axis + 1:]
    return values.at[tuple(place)].set(least).at[tuple(beside)].set(top_value)


def block_levels(rng, shape, shards, least, largest):
    def one(dim, shards_of):
        steps = jax.random.uniform(jax.random.fold_in(jax.random.fold_in(rng, 6), dim), (shards_of,), jnp.float32, least / len(shards), largest / len(shards))
        return jnp.repeat(jnp.exp(steps), shape[dim] // shards_of).reshape((-1,) + (1,) * (len(shape) - dim - 1))

    factor_of = one(*shards[0])
    for cut in shards[1:]:
        factor_of = factor_of * one(*cut)
    return factor_of


def centred(rng, dims, width, bound, cuts=(), kind=jnp.bfloat16):
    array = jax.random.normal(rng, dims, jnp.float32) * width
    if len(cuts) > 0:
        array = block_levels(rng, dims, cuts, -0.22, 0.18) * array
    return jnp.clip(array, min=-bound, max=bound).astype(kind)


def setup_inputs(seed: int = 0) -> dict:
    key_list = jax.random.split(jax.random.key(seed), 10)
    hidden = centred(key_list[0], (N_EXPERT, TOKROWS, FF_DEV), 1.0, 6.0, ((0, 16), (1, 16)))
    outgrad = centred(key_list[1], (N_EXPERT, TOKROWS, D), 1.0, 6.0, ((0, 16), (1, 16)))
    row_expert = place_ends(jax.random.randint(key_list[2], (N_EXPERT, TOKROWS), 0, EXP_WIN), jax.random.fold_in(key_list[2], 1), 0, EXP_WIN - 1).astype(jnp.int32)
    counts = draw_counts(jax.random.fold_in(key_list[9], 71), 0)
    learner_map = draw_learner_map(jax.random.fold_in(key_list[9], 71), 0)
    rollout_map = draw_rollout_map(jax.random.fold_in(key_list[9], 71), 0)
    master = centred(key_list[6], (D, UNITS * BLOCK), 0.5, 3.0, ((0, 16), (1, 16)), jnp.float32)
    moment1 = centred(key_list[7], (D, UNITS * BLOCK), 2.0, 12.0, ((0, 16), (1, 16)), jnp.float32)
    moment2 = jnp.clip(jnp.exp(math.log(1000.0) - 6.9077553 * jax.random.uniform(key_list[8], (D, UNITS * BLOCK), jnp.float32) ** block_levels(key_list[8], (D, UNITS * BLOCK), ((0, 16), (1, 16)), -0.2, 0.2)), 1.0, 1000.0)
    return {"hidden": hidden, "outgrad": outgrad, "row_expert": row_expert, "counts": counts, "learner_map": learner_map, "rollout_map": rollout_map, "master": master, "moment1": moment1, "moment2": moment2}


beta_one = 0.9
beta_two = 0.95
learn_rate = 0.01
decay_rate = 0.1
epsilon = 1e-08
step_count = 100.0

def reference(hidden, outgrad, row_expert, counts, learner_map, rollout_map, master, moment1, moment2):
    groups = N_EXPERT
    block_width = hidden.shape[2] // groups
    per_expert = FF // block_width
    slot_expert = (learner_map // per_expert).reshape(groups, groups)
    row_index = jnp.arange(hidden.shape[1], dtype=jnp.int32)

    def one_group(index):
        live_rows = row_index % ROWS < counts[index][row_index // ROWS]
        kept = live_rows[:, None] & (row_expert[index][:, None] == slot_expert[index][None, :])
        kept_cols = jnp.repeat(kept, block_width, axis=1)
        masked = jnp.where(kept_cols, hidden[index], jnp.zeros((), hidden.dtype))
        return jnp.dot(outgrad[index].T, masked, preferred_element_type=jnp.float32)
    partials = lax.map(one_group, jnp.arange(groups, dtype=jnp.int32))
    gradient = jnp.moveaxis(partials, 0, 1).reshape(master.shape)
    new_moment1 = beta_one * moment1 + (1.0 - beta_one) * gradient
    new_moment2 = beta_two * moment2 + (1.0 - beta_two) * gradient * gradient
    bias_one = 1.0 - beta_one ** step_count
    bias_two = 1.0 - beta_two ** step_count
    update = new_moment1 / bias_one / (jnp.sqrt(new_moment2 / bias_two) + epsilon)
    new_master = master - learn_rate * (update + decay_rate * master)
    rounded = new_master.astype(jnp.bfloat16).reshape(master.shape[0], groups * groups, block_width)
    position = jnp.argsort(learner_map)[rollout_map].astype(jnp.int32)
    rollout_weights = jnp.take(rounded, position, axis=1).reshape(master.shape)
    return (new_master, new_moment1, new_moment2, rollout_weights)
```

```python
import jax
import jax.numpy as jnp
from jax import lax
from jax.experimental import pallas as pl
from jax.experimental.pallas import tpu as pltpu
from jax.sharding import PartitionSpec as P

MESH = pl.DeviceIdType.MESH
FF = 14336
D = 4096
COLS = 1792
UNIT = 112
GROUPS = 16
HALF_UNITS = FF // UNIT
TOK = 128
CHUNKS = 4
CROWS = TOK // CHUNKS
WIDTH = 256
TILE = 256

beta_one = 0.9
beta_two = 0.95
learn_rate = 0.01
decay_rate = 0.1
epsilon = 1e-08
step_count = 100.0


def dp_of(x, plane, core):
    return (lax.rem(x + 4, 4) * 2 + plane) * 2 + core


def gather_kernel(
    hid_ref, og_ref, rexp_ref, lrow_ref, rrow_ref, count_ref, lsm_ref, rsm_ref,
    grad_ref, index_ref,
    hid, og, abuf, bbuf, abuf_t,
    load_sem, a_send, a_recv, z_send, z_recv, x_send, x_recv, o_send, o_recv, s_send, s_recv,
):
    dp = lax.axis_index("dp")
    ex = lax.axis_index("expert")
    core = lax.rem(dp, 2)
    plane = lax.rem(dp // 2, 2)
    x = dp // 4
    planes = (plane, 1 - plane)

    load_h = pltpu.make_async_copy(hid_ref, hid, load_sem.at[0])
    load_o = pltpu.make_async_copy(og_ref, og, load_sem.at[1])
    load_h.start()
    load_o.start()
    barrier = pltpu.get_barrier_semaphore()
    for k in range(1, 16):
        pl.semaphore_signal(barrier, inc=1, device_id=(lax.rem(dp + k, 16), ex), device_id_type=MESH)

    lane = lax.broadcasted_iota(jnp.int32, (8, COLS), 1)
    unit_of = jnp.zeros((8, COLS), jnp.int32)
    for u in range(GROUPS):
        belongs = (lane >= u * UNIT) & (lane < (u + 1) * UNIT)
        unit_of = jnp.where(belongs, lsm_ref[ex * GROUPS + u], unit_of)
    expert_of = jnp.where(unit_of >= HALF_UNITS, 1, 0)[0:1, :]
    rows = lax.broadcasted_iota(jnp.int32, (TOK, TOK), 0)
    cols = lax.broadcasted_iota(jnp.int32, (TOK, TOK), 1)
    row_expert = jnp.sum(jnp.where(rows == cols, rexp_ref[...], 0), axis=1, keepdims=True)
    live = lax.broadcasted_iota(jnp.int32, (TOK, 1), 0) < count_ref[0, 0]
    row_key = jnp.where(live, row_expert, -1)
    load_h.wait()
    for j in range(CHUNKS):
        key = row_key[j * CROWS : (j + 1) * CROWS]
        kept = key == expert_of
        block = hid[j * CROWS : (j + 1) * CROWS, :].astype(jnp.float32)
        bbuf[plane, j, x * 2 + core] = jnp.where(kept, block, 0.0).astype(jnp.bfloat16)

    wide = lax.broadcasted_iota(jnp.int32, (GROUPS, 256), 1) // GROUPS
    high = lax.broadcasted_iota(jnp.int32, (GROUPS, 1), 0)
    held = jnp.zeros((GROUPS, 1), jnp.int32)
    wanted = jnp.zeros((GROUPS, 1), jnp.int32)
    for u in range(GROUPS):
        held = jnp.where(high == u, lsm_ref[ex * GROUPS + u], held)
        wanted = jnp.where(high == u, rsm_ref[ex * GROUPS + u], wanted)
    target = jnp.sum(jnp.where(rrow_ref[...] == held, wide, 0), axis=1, keepdims=True)
    source = jnp.sum(jnp.where(lrow_ref[...] == wanted, wide, 0), axis=1, keepdims=True)
    low = lax.broadcasted_iota(jnp.int32, (GROUPS, 128), 1)
    high = lax.broadcasted_iota(jnp.int32, (GROUPS, 128), 0)
    order_row = jnp.sum(jnp.where(target == low, high, 0), axis=0, keepdims=True)
    source_row = jnp.sum(jnp.where(high == low, source, 0), axis=0, keepdims=True)
    index_ref[0:1, :] = order_row
    index_ref[1:2, :] = source_row

    load_o.wait()
    pl.semaphore_wait(barrier, 15)

    started = []

    def send(src, dst, ssem, rsem, target_dp):
        copy = pltpu.make_async_remote_copy(
            src_ref=src, dst_ref=dst, send_sem=ssem, recv_sem=rsem,
            device_id=(target_dp, ex), device_id_type=MESH,
        )
        copy.start()
        started.append(copy)

    def arrived(ref, rsem):
        pltpu.make_async_copy(ref, ref, rsem).wait()

    def send_a(other):
        cut = og.at[:, :, pl.ds(pl.multiple_of(other * WIDTH, WIDTH), WIDTH)]
        send(cut, abuf.at[plane, :, x * 2 + core], a_send.at[other], a_recv.at[dp], other)

    for dx in (0, 1, 3, 2):
        for dc in range(2):
            send_a(dp_of(x + dx, 1 - plane, lax.rem(core + dc, 2)))

    def slot(p, j, dx, c):
        return bbuf.at[planes[p], j, lax.rem(x + dx + 4, 4) * 2 + c]

    def center(p, j):
        me = slot(p, j, 0, core)
        send(me, me, x_send.at[p, j, 0], x_recv.at[p, j, 0], dp_of(x + 1, plane, core))
        send(me, me, x_send.at[p, j, 1], x_recv.at[p, j, 1], dp_of(x - 1, plane, core))
        send(me, me, s_send.at[p, j, 0], s_recv.at[p, j, 0], dp_of(x, plane, 1 - core))

    def z_out(j):
        me = slot(0, j, 0, core)
        send(me, me, z_send.at[j], z_recv.at[j], dp_of(x, 1 - plane, core))

    def z_in(j):
        arrived(slot(1, j, 0, core), z_recv.at[j])
        center(1, j)

    def sides(p, j):
        left = slot(p, j, -1, core)
        arrived(left, x_recv.at[p, j, 0])
        first = left.at[pl.ds(0, CROWS // 2)]
        send(first, first, o_send.at[p, j, 0], o_recv.at[p, j, 0], dp_of(x + 1, plane, core))
        send(left, left, s_send.at[p, j, 1], s_recv.at[p, j, 1], dp_of(x, plane, 1 - core))
        right = slot(p, j, 1, core)
        arrived(right, x_recv.at[p, j, 1])
        second = right.at[pl.ds(CROWS // 2, CROWS // 2)]
        send(second, second, o_send.at[p, j, 1], o_recv.at[p, j, 1], dp_of(x - 1, plane, core))
        send(right, right, s_send.at[p, j, 2], s_recv.at[p, j, 2], dp_of(x, plane, 1 - core))

    def opposite(p, j):
        far = slot(p, j, 2, core)
        arrived(far.at[pl.ds(0, CROWS // 2)], o_recv.at[p, j, 0])
        arrived(far.at[pl.ds(CROWS // 2, CROWS // 2)], o_recv.at[p, j, 1])
        send(far, far, s_send.at[p, j, 3], s_recv.at[p, j, 3], dp_of(x, plane, 1 - core))

    def wait_a(p):
        for dx in range(4):
            for dc in range(2):
                if (p, dx, dc) == (0, 0, 0):
                    continue
                c = lax.rem(core + dc, 2)
                src = dp_of(x + dx, planes[p], c)
                arrived(abuf.at[planes[p], :, lax.rem(x + dx, 4) * 2 + c], a_recv.at[src])

    def compute(p, j):
        for i, dx in enumerate((0, -1, 1, 2)):
            arrived(slot(p, j, dx, 1 - core), s_recv.at[p, j, i])
        lhs = abuf[planes[p], j].reshape(8 * CROWS, WIDTH)
        abuf_t[...] = jnp.transpose(lhs)

        def tile(t, carry):
            at = pl.ds(pl.multiple_of(t * TILE, TILE), TILE)
            rhs = bbuf[planes[p], j, :, :, at].reshape(8 * CROWS, TILE)
            part = jnp.dot(abuf_t[...], rhs, preferred_element_type=jnp.float32)
            if (p, j) == (0, 0):
                grad_ref[:, at] = part
            else:
                grad_ref[:, at] += part
            return carry

        lax.fori_loop(0, COLS // TILE, tile, 0)

    for j in range(CHUNKS):
        z_out(j)
        center(0, j)
    for dx in (1, 3, 2, 0):
        for dc in range(2):
            if (dx, dc) != (0, 0):
                send_a(dp_of(x + dx, plane, lax.rem(core + dc, 2)))
    cols_own = pl.ds(pl.multiple_of(dp * WIDTH, WIDTH), WIDTH)
    for j in range(CHUNKS):
        abuf[plane, j, x * 2 + core] = og[j, :, cols_own]

    blocks = [(p, j) for p in range(2) for j in range(CHUNKS)]
    n = len(blocks)
    for i in range(n + 2):
        if i < n:
            sides(*blocks[i])
        if 1 <= i <= n:
            opposite(*blocks[i - 1])
        if i >= 2:
            if i - 2 == 0:
                wait_a(0)
            if i - 2 == CHUNKS:
                wait_a(1)
            compute(*blocks[i - 2])
        if i + 1 < n and blocks[i + 1][0] == 1:
            z_in(blocks[i + 1][1])
    for copy in started:
        copy.wait_send()


def gather_call(hidden, outgrad, row_expert, counts, learner_map, rollout_map):
    vmem = pl.BlockSpec(memory_space=pltpu.VMEM)
    smem = pl.BlockSpec(memory_space=pltpu.SMEM)
    hbm = pl.BlockSpec(memory_space=pl.ANY)
    dma = pltpu.SemaphoreType.DMA
    return pl.pallas_call(
        gather_kernel,
        name="gather_multiply",
        out_shape=(
            jax.ShapeDtypeStruct((WIDTH, COLS), jnp.float32),
            jax.ShapeDtypeStruct((2, 128), jnp.int32),
        ),
        in_specs=[hbm, hbm, vmem, vmem, vmem, smem, smem, smem],
        out_specs=(vmem, vmem),
        scratch_shapes=[
            pltpu.VMEM((TOK, COLS), jnp.bfloat16),
            pltpu.VMEM((CHUNKS, CROWS, D), jnp.bfloat16),
            pltpu.VMEM((2, CHUNKS, 8, CROWS, WIDTH), jnp.bfloat16),
            pltpu.VMEM((2, CHUNKS, 8, CROWS, COLS), jnp.bfloat16),
            pltpu.VMEM((WIDTH, 8 * CROWS), jnp.bfloat16),
            dma((3,)),
            dma((16,)), dma((16,)),
            dma((CHUNKS,)), dma((CHUNKS,)),
            dma((2, CHUNKS, 2)), dma((2, CHUNKS, 2)),
            dma((2, CHUNKS, 2)), dma((2, CHUNKS, 2)),
            dma((2, CHUNKS, 4)), dma((2, CHUNKS, 4)),
        ],
        compiler_params=pltpu.CompilerParams(
            collective_id=0, has_side_effects=True, vmem_limit_bytes=32 * 1024 * 1024
        ),
    )(
        hidden,
        outgrad.reshape(CHUNKS, CROWS, D),
        row_expert,
        learner_map.reshape(1, 256),
        rollout_map.reshape(1, 256),
        counts,
        learner_map,
        rollout_map,
    )


PACKED = 224
FOLD = 32
LANES = 128


def spread_kernel(index_ref, val_ref, out_ref, packed, sends, recvs, send_sem, recv_sem):
    dp = lax.axis_index("dp")
    ex = lax.axis_index("expert")
    barrier = pltpu.get_barrier_semaphore()
    for k in range(1, GROUPS):
        pl.semaphore_signal(
            barrier, inc=1, device_id=(dp, lax.rem(ex + k, GROUPS)), device_id_type=MESH
        )
    lane = lax.broadcasted_iota(jnp.int32, (FOLD, LANES), 1)
    lane_all = lax.broadcasted_iota(jnp.int32, (WIDTH, LANES), 1)

    def shifted(value, by):
        by = by % LANES
        return value if by == 0 else pltpu.roll(value, by, 1)

    for u in range(GROUPS):
        block, off = divmod(u * UNIT, LANES)
        one = shifted(val_ref[:, block * LANES : (block + 1) * LANES], -off)
        if off + UNIT > LANES:
            two = shifted(val_ref[:, (block + 1) * LANES : (block + 2) * LANES], -off)
            one = jnp.where(lane_all < LANES - off, one, two)
        last = one[PACKED:]
        for g in range(PACKED // FOLD):
            extra = shifted(last, UNIT - 16 * g)
            mine = one[g * FOLD : (g + 1) * FOLD]
            packed[u, g * FOLD : (g + 1) * FOLD, :] = jnp.where(lane < UNIT, mine, extra)

    def to_slot(k, carry):
        sends[k] = packed[index_ref[0, lax.rem(ex + k, GROUPS)]]
        return carry

    lax.fori_loop(0, GROUPS, to_slot, 0)
    pl.semaphore_wait(barrier, GROUPS - 1)
    copies = []
    for k in range(1, GROUPS):
        to = lax.rem(ex + k, GROUPS)
        copy = pltpu.make_async_remote_copy(
            src_ref=sends.at[k], dst_ref=recvs.at[ex],
            send_sem=send_sem.at[k], recv_sem=recv_sem.at[k],
            device_id=(dp, to), device_id_type=MESH,
        )
        copy.start()
        copies.append(copy)
    recvs[ex] = sends[0]
    for k in range(1, GROUPS):
        came = recvs.at[lax.rem(ex - k + GROUPS, GROUPS)]
        pltpu.make_async_copy(came, came, recv_sem.at[k]).wait()

    def unfolded(p):
        data = recvs[index_ref[1, p]]
        tail = jnp.zeros((FOLD, LANES), data.dtype)
        for g in range(PACKED // FOLD):
            moved = shifted(data[g * FOLD : (g + 1) * FOLD], 16 * g - UNIT)
            tail = jnp.where((lane >= 16 * g) & (lane < 16 * g + 16), moved, tail)
        return jnp.concatenate([data, tail], axis=0)

    held = unfolded(0)
    pos = 0
    for q in range(COLS // LANES):
        off = q * LANES - pos * UNIT
        nxt = unfolded(pos + 1)
        a = shifted(held, -off)
        b = shifted(nxt, UNIT - off)
        out_ref[:, q * LANES : (q + 1) * LANES] = jnp.where(lane_all < UNIT - off, a, b)
        pos += 1
        held = nxt
        if (q + 1) * LANES - pos * UNIT == UNIT and pos + 1 < GROUPS:
            pos += 1
            held = unfolded(pos)
    for copy in copies:
        copy.wait_send()


def spread_call(index, value):
    vmem = pl.BlockSpec(memory_space=pltpu.VMEM)
    dma = pltpu.SemaphoreType.DMA
    return pl.pallas_call(
        spread_kernel,
        name="spread_units",
        out_shape=jax.ShapeDtypeStruct((WIDTH, COLS), jnp.bfloat16),
        in_specs=[pl.BlockSpec(memory_space=pltpu.SMEM), vmem],
        out_specs=vmem,
        scratch_shapes=[
            pltpu.VMEM((GROUPS, PACKED, LANES), jnp.bfloat16),
            pltpu.VMEM((GROUPS, PACKED, LANES), jnp.bfloat16),
            pltpu.VMEM((GROUPS, PACKED, LANES), jnp.bfloat16),
            dma((GROUPS,)), dma((GROUPS,)),
        ],
        compiler_params=pltpu.CompilerParams(
            collective_id=1, has_side_effects=True, vmem_limit_bytes=16 * 1024 * 1024
        ),
    )(index, value)


def on_device(
    hidden, outgrad, row_expert, counts, learner_map, rollout_map, master, moment1, moment2
):
    gradient, index = gather_call(
        hidden[0], outgrad[0], row_expert, counts, learner_map, rollout_map
    )
    new_moment1 = beta_one * moment1 + (1.0 - beta_one) * gradient
    new_moment2 = beta_two * moment2 + (1.0 - beta_two) * gradient * gradient
    bias_one = 1.0 - beta_one**step_count
    bias_two = 1.0 - beta_two**step_count
    update = new_moment1 / bias_one / (jnp.sqrt(new_moment2 / bias_two) + epsilon)
    new_master = master - learn_rate * (update + decay_rate * master)
    rollout_weights = spread_call(index, new_master.astype(jnp.bfloat16))
    return (new_master, new_moment1, new_moment2, rollout_weights)


def solution(mesh):
    return jax.shard_map(
        on_device,
        mesh=mesh,
        in_specs=(
            P("expert", "dp", None),
            P("expert", "dp", None),
            P("expert", "dp"),
            P("expert", "dp"),
            P(),
            P(),
            P("dp", "expert"),
            P("dp", "expert"),
            P("dp", "expert"),
        ),
        out_specs=(P("dp", "expert"),) * 4,
        check_vma=False,
    )
```

```python
import jax
import jax.numpy as jnp
from jax import lax
from jax.experimental import pallas as pl
from jax.experimental.pallas import tpu as pltpu
from jax.sharding import PartitionSpec as P

MESH = pl.DeviceIdType.MESH
FF = 14336
D = 4096
COLS = 1792
UNIT = 112
GROUPS = 16
HALF_UNITS = FF // UNIT
TOK = 128
CHUNKS = 4
CROWS = TOK // CHUNKS
WIDTH = 256
TILE = 256
PARTS = 2
DROWS = WIDTH // PARTS
FOLD = 16
PACKED = DROWS - FOLD
LANES = 128

beta_one = 0.9
beta_two = 0.95
learn_rate = 0.01
decay_rate = 0.1
epsilon = 1e-08
step_count = 100.0


def dp_of(x, plane, core):
    return (lax.rem(x + 4, 4) * 2 + plane) * 2 + core


def step_kernel(
    hid_ref, og_ref, rexp_ref, lrow_ref, rrow_ref, count_ref, lsm_ref, rsm_ref,
    master_ref, mom1_ref, mom2_ref,
    new_master, new_mom1, new_mom2, out_ref,
    hid, og, rexp, lrow, rrow, master, mom1, mom2, abuf, bbuf, lhs_t, grad,
    index_v, index, value, packed, sends, recv_0, recv_1,
    load_sem, a_send, a_recv, z_send, z_recv, x_send, x_recv, o_send, o_recv, s_send, s_recv,
    e_send, e_recv,
):
    recvs = (recv_0, recv_1)
    dp = lax.axis_index("dp")
    ex = lax.axis_index("expert")
    core = lax.rem(dp, 2)
    plane = lax.rem(dp // 2, 2)
    x = dp // 4
    planes = (plane, 1 - plane)

    loads = [
        pltpu.make_async_copy(src, dst, load_sem.at[i])
        for i, (src, dst) in enumerate(
            (
                (hid_ref, hid), (rexp_ref, rexp), (lrow_ref, lrow), (rrow_ref, rrow), (og_ref, og),
                (mom1_ref, mom1), (mom2_ref, mom2), (master_ref, master),
            )
        )
    ]
    for load in loads:
        load.start()
    barrier = pltpu.get_barrier_semaphore()
    for k in range(1, 16):
        pl.semaphore_signal(barrier, inc=1, device_id=(lax.rem(dp + k, 16), ex), device_id_type=MESH)
    for k in range(1, 16):
        pl.semaphore_signal(barrier, inc=1, device_id=(dp, lax.rem(ex + k, 16)), device_id_type=MESH)

    lane = lax.broadcasted_iota(jnp.int32, (8, COLS), 1)
    unit_of = jnp.zeros((8, COLS), jnp.int32)
    for u in range(GROUPS):
        belongs = (lane >= u * UNIT) & (lane < (u + 1) * UNIT)
        unit_of = jnp.where(belongs, lsm_ref[ex * GROUPS + u], unit_of)
    expert_of = jnp.where(unit_of >= HALF_UNITS, 1, 0)[0:1, :]
    rows = lax.broadcasted_iota(jnp.int32, (TOK, TOK), 0)
    cols = lax.broadcasted_iota(jnp.int32, (TOK, TOK), 1)
    for load in loads[:4]:
        load.wait()
    row_expert = jnp.sum(jnp.where(rows == cols, rexp[...], 0), axis=1, keepdims=True)
    live = lax.broadcasted_iota(jnp.int32, (TOK, 1), 0) < count_ref[0, 0]
    row_key = jnp.where(live, row_expert, -1)
    for j in range(CHUNKS):
        key = row_key[j * CROWS : (j + 1) * CROWS]
        kept = key == expert_of
        block = hid[j * CROWS : (j + 1) * CROWS, :].astype(jnp.float32)
        bbuf[plane, j, x * 2 + core] = jnp.where(kept, block, 0.0).astype(jnp.bfloat16)
    loads[4].wait()
    pl.semaphore_wait(barrier, 30)

    started = []

    def send(src, dst, ssem, rsem, to):
        copy = pltpu.make_async_remote_copy(
            src_ref=src, dst_ref=dst, send_sem=ssem, recv_sem=rsem,
            device_id=to, device_id_type=MESH,
        )
        copy.start()
        started.append(copy)

    def arrived(ref, rsem):
        pltpu.make_async_copy(ref, ref, rsem).wait()

    def a_columns(k, other):
        return pl.ds(pl.multiple_of(other * WIDTH + k * DROWS, DROWS), DROWS)

    def send_a(k, other):
        cut = og.at[:, :, a_columns(k, other)]
        slot_a = abuf.at[k, plane, :, x * 2 + core]
        send(cut, slot_a, a_send.at[k, other], a_recv.at[k, dp], (other, ex))

    def all_a(k):
        for dx in (0, 1, 3, 2):
            for dc in range(2):
                c = lax.rem(core + dc, 2)
                send_a(k, dp_of(x + dx, 1 - plane, c))
                if (dx, dc) != (0, 0):
                    send_a(k, dp_of(x + dx, plane, c))

    def slot(p, j, dx, c):
        return bbuf.at[planes[p], j, lax.rem(x + dx + 4, 4) * 2 + c]

    def peer(dx, c):
        return (dp_of(x + dx, plane, c), ex)

    def center(p, j):
        me = slot(p, j, 0, core)
        send(me, me, x_send.at[p, j, 0], x_recv.at[p, j, 0], peer(1, core))
        send(me, me, x_send.at[p, j, 1], x_recv.at[p, j, 1], peer(-1, core))
        send(me, me, s_send.at[p, j, 0], s_recv.at[p, j, 0], peer(0, 1 - core))

    def z_out(j):
        me = slot(0, j, 0, core)
        send(me, me, z_send.at[j], z_recv.at[j], (dp_of(x, 1 - plane, core), ex))

    def z_in(j):
        arrived(slot(1, j, 0, core), z_recv.at[j])
        center(1, j)

    def sides(p, j):
        left = slot(p, j, -1, core)
        arrived(left, x_recv.at[p, j, 0])
        first = left.at[pl.ds(0, CROWS // 2)]
        send(first, first, o_send.at[p, j, 0], o_recv.at[p, j, 0], peer(1, core))
        send(left, left, s_send.at[p, j, 1], s_recv.at[p, j, 1], peer(0, 1 - core))
        right = slot(p, j, 1, core)
        arrived(right, x_recv.at[p, j, 1])
        second = right.at[pl.ds(CROWS // 2, CROWS // 2)]
        send(second, second, o_send.at[p, j, 1], o_recv.at[p, j, 1], peer(-1, core))
        send(right, right, s_send.at[p, j, 2], s_recv.at[p, j, 2], peer(0, 1 - core))

    def opposite(p, j):
        far = slot(p, j, 2, core)
        arrived(far.at[pl.ds(0, CROWS // 2)], o_recv.at[p, j, 0])
        arrived(far.at[pl.ds(CROWS // 2, CROWS // 2)], o_recv.at[p, j, 1])
        send(far, far, s_send.at[p, j, 3], s_recv.at[p, j, 3], peer(0, 1 - core))

    def wait_a(k, p):
        for dx in range(4):
            for dc in range(2):
                if (p, dx, dc) == (0, 0, 0):
                    continue
                c = lax.rem(core + dc, 2)
                src = dp_of(x + dx, planes[p], c)
                arrived(abuf.at[k, planes[p], :, lax.rem(x + dx, 4) * 2 + c], a_recv.at[k, src])

    def wait_sibling(p):
        for j in range(CHUNKS):
            for i, dx in enumerate((0, -1, 1, 2)):
                arrived(slot(p, j, dx, 1 - core), s_recv.at[p, j, i])

    def multiply(k, p):
        lhs = abuf[k, planes[p]].reshape(8 * TOK, DROWS)
        lhs_t[...] = jnp.transpose(lhs)

        def tile(t, carry):
            at = pl.ds(pl.multiple_of(t * TILE, TILE), TILE)
            rhs = bbuf[planes[p], :, :, :, at].reshape(8 * TOK, TILE)
            part = jnp.dot(lhs_t[...], rhs, preferred_element_type=jnp.float32)
            if p == 0:
                grad[:, at] = part
            else:
                grad[:, at] += part
            return carry

        lax.fori_loop(0, COLS // TILE, tile, 0)

    bias_one = 1.0 - beta_one**step_count
    bias_two = 1.0 - beta_two**step_count

    def update(k):
        def piece(i, carry):
            r = pl.multiple_of(lax.rem(i, DROWS // 32) * 32, 32)
            at = pl.ds(pl.multiple_of((i // (DROWS // 32)) * TILE, TILE), TILE)
            here = (pl.ds(k * DROWS + r, 32), at)
            g = grad[pl.ds(r, 32), at]
            m1 = beta_one * mom1[here] + (1.0 - beta_one) * g
            m2 = beta_two * mom2[here] + (1.0 - beta_two) * g * g
            w = master[here]
            step = m1 * (1.0 / bias_one) / (jnp.sqrt(m2 * (1.0 / bias_two)) + epsilon)
            w = w - learn_rate * (step + decay_rate * w)
            new_mom1[here] = m1
            new_mom2[here] = m2
            new_master[here] = w
            value[pl.ds(r, 32), at] = w.astype(jnp.bfloat16)
            return carry

        lax.fori_loop(0, (DROWS // 32) * (COLS // TILE), piece, 0)

    lane_fold = lax.broadcasted_iota(jnp.int32, (FOLD, LANES), 1)
    lane_all = lax.broadcasted_iota(jnp.int32, (DROWS, LANES), 1)

    def shifted(val, by):
        by = by % LANES
        return val if by == 0 else pltpu.roll(val, by, 1)

    def pack():
        for u in range(GROUPS):
            block, off = divmod(u * UNIT, LANES)
            one = shifted(value[:, block * LANES : (block + 1) * LANES], -off)
            if off + UNIT > LANES:
                two = shifted(value[:, (block + 1) * LANES : (block + 2) * LANES], -off)
                one = jnp.where(lane_all < LANES - off, one, two)
            last = one[PACKED:]
            for g in range(PACKED // FOLD):
                extra = shifted(last, UNIT - 16 * g)
                mine = one[g * FOLD : (g + 1) * FOLD]
                packed[u, g * FOLD : (g + 1) * FOLD, :] = jnp.where(lane_fold < UNIT, mine, extra)

    def spread(k):
        def to_slot(i, carry):
            sends[k, i] = packed[index[0, lax.rem(ex + i, GROUPS)]]
            return carry

        lax.fori_loop(0, GROUPS, to_slot, 0)
        for i in range(1, GROUPS):
            to = lax.rem(ex + i, GROUPS)
            send(sends.at[k, i], recvs[k].at[ex], e_send.at[k, i], e_recv.at[k, i], (dp, to))
        recvs[k][ex] = sends[k, 0]

    def collect(k):
        for i in range(1, GROUPS):
            arrived(recvs[k].at[lax.rem(ex - i + GROUPS, GROUPS)], e_recv.at[k, i])

        def unfolded(p):
            data = recvs[k][index[1, p]]
            tail = jnp.zeros((FOLD, LANES), data.dtype)
            for g in range(PACKED // FOLD):
                moved = shifted(data[g * FOLD : (g + 1) * FOLD], 16 * g - UNIT)
                tail = jnp.where((lane_fold >= 16 * g) & (lane_fold < 16 * g + 16), moved, tail)
            return jnp.concatenate([data, tail], axis=0)

        held = unfolded(0)
        pos = 0
        for q in range(COLS // LANES):
            off = q * LANES - pos * UNIT
            nxt = unfolded(pos + 1)
            a = shifted(held, -off)
            b = shifted(nxt, UNIT - off)
            joined = jnp.where(lane_all < UNIT - off, a, b)
            out_ref[k * DROWS : (k + 1) * DROWS, q * LANES : (q + 1) * LANES] = joined
            pos += 1
            held = nxt
            if (q + 1) * LANES - pos * UNIT == UNIT and pos + 1 < GROUPS:
                pos += 1
                held = unfolded(pos)

    for j in range(CHUNKS):
        z_out(j)
        center(0, j)
    all_a(0)
    for k in range(PARTS):
        for j in range(CHUNKS):
            abuf[k, plane, j, x * 2 + core] = og[j, :, a_columns(k, dp)]

    wide = lax.broadcasted_iota(jnp.int32, (GROUPS, 256), 1) // GROUPS
    high = lax.broadcasted_iota(jnp.int32, (GROUPS, 1), 0)
    have = jnp.zeros((GROUPS, 1), jnp.int32)
    wanted = jnp.zeros((GROUPS, 1), jnp.int32)
    for u in range(GROUPS):
        have = jnp.where(high == u, lsm_ref[ex * GROUPS + u], have)
        wanted = jnp.where(high == u, rsm_ref[ex * GROUPS + u], wanted)
    target = jnp.max(jnp.where(rrow[...] == have, wide, 0), axis=1, keepdims=True)
    source = jnp.max(jnp.where(lrow[...] == wanted, wide, 0), axis=1, keepdims=True)
    low = lax.broadcasted_iota(jnp.int32, (GROUPS, 128), 1)
    high = lax.broadcasted_iota(jnp.int32, (GROUPS, 128), 0)
    index_v[0:1, :] = jnp.max(jnp.where(target == low, high, 0), axis=0, keepdims=True)
    index_v[1:2, :] = jnp.max(jnp.where(high == low, source, 0), axis=0, keepdims=True)
    to_scalar = pltpu.make_async_copy(index_v, index, load_sem.at[8])

    sides(0, 0)
    sides(0, 1)
    to_scalar.start()
    z_in(0)
    sides(0, 2)
    sides(0, 3)
    z_in(1)
    opposite(0, 0)
    opposite(0, 1)
    z_in(2)
    opposite(0, 2)
    opposite(0, 3)
    sides(1, 0)
    z_in(3)
    all_a(1)
    sides(1, 1)
    sides(1, 2)
    sides(1, 3)
    to_scalar.wait()
    for load in loads[5:]:
        load.wait()
    wait_sibling(0)
    wait_a(0, 0)
    multiply(0, 0)
    for j in range(CHUNKS):
        opposite(1, j)
    wait_sibling(1)
    wait_a(0, 1)
    multiply(0, 1)
    update(0)
    pack()
    spread(0)
    wait_a(1, 0)
    multiply(1, 0)
    wait_a(1, 1)
    multiply(1, 1)
    update(1)
    pack()
    spread(1)
    collect(0)
    collect(1)
    for copy in started:
        copy.wait_send()


def step_call(hidden, outgrad, row_expert, counts, learner_map, rollout_map, master, mom1, mom2):
    vmem = pl.BlockSpec(memory_space=pltpu.VMEM)
    smem = pl.BlockSpec(memory_space=pltpu.SMEM)
    hbm = pl.BlockSpec(memory_space=pltpu.HBM)
    dma = pltpu.SemaphoreType.DMA
    state = pltpu.VMEM((WIDTH, COLS), jnp.float32)

    def far(value):
        return pltpu.with_memory_space_constraint(value, pltpu.HBM)

    return pl.pallas_call(
        step_kernel,
        name="grad_update_spread",
        out_shape=(state, state, state, pltpu.VMEM((WIDTH, COLS), jnp.bfloat16)),
        in_specs=[hbm, hbm, hbm, hbm, hbm, smem, smem, smem, hbm, hbm, hbm],
        out_specs=(vmem, vmem, vmem, vmem),
        scratch_shapes=[
            pltpu.VMEM((TOK, COLS), jnp.bfloat16),
            pltpu.VMEM((CHUNKS, CROWS, D), jnp.bfloat16),
            pltpu.VMEM((1, TOK), jnp.int32),
            pltpu.VMEM((1, 256), jnp.int32),
            pltpu.VMEM((1, 256), jnp.int32),
            pltpu.VMEM((WIDTH, COLS), jnp.float32),
            pltpu.VMEM((WIDTH, COLS), jnp.float32),
            pltpu.VMEM((WIDTH, COLS), jnp.float32),
            pltpu.VMEM((PARTS, 2, CHUNKS, 8, CROWS, DROWS), jnp.bfloat16),
            pltpu.VMEM((2, CHUNKS, 8, CROWS, COLS), jnp.bfloat16),
            pltpu.VMEM((DROWS, 8 * TOK), jnp.bfloat16),
            pltpu.VMEM((DROWS, COLS), jnp.float32),
            pltpu.VMEM((2, 128), jnp.int32),
            pltpu.SMEM((2, 128), jnp.int32),
            pltpu.VMEM((DROWS, COLS), jnp.bfloat16),
            pltpu.VMEM((GROUPS, PACKED, LANES), jnp.bfloat16),
            pltpu.VMEM((PARTS, GROUPS, PACKED, LANES), jnp.bfloat16),
            pltpu.VMEM((GROUPS, PACKED, LANES), jnp.bfloat16),
            pltpu.VMEM((GROUPS, PACKED, LANES), jnp.bfloat16),
            dma((9,)),
            dma((PARTS, 16)), dma((PARTS, 16)),
            dma((CHUNKS,)), dma((CHUNKS,)),
            dma((2, CHUNKS, 2)), dma((2, CHUNKS, 2)),
            dma((2, CHUNKS, 2)), dma((2, CHUNKS, 2)),
            dma((2, CHUNKS, 4)), dma((2, CHUNKS, 4)),
            dma((PARTS, GROUPS)), dma((PARTS, GROUPS)),
        ],
        compiler_params=pltpu.CompilerParams(
            collective_id=0, has_side_effects=True, vmem_limit_bytes=40 * 1024 * 1024
        ),
    )(
        far(hidden),
        far(outgrad.reshape(CHUNKS, CROWS, D)),
        far(row_expert),
        far(learner_map.reshape(1, 256)),
        far(rollout_map.reshape(1, 256)),
        counts,
        learner_map,
        rollout_map,
        far(master),
        far(mom1),
        far(mom2),
    )


def land_kernel(*refs):
    ins, outs, sem = refs[:4], refs[4:8], refs[8]
    copies = [pltpu.make_async_copy(a, b, sem.at[i]) for i, (a, b) in enumerate(zip(ins, outs))]
    for copy in copies:
        copy.start()
    for copy in copies:
        copy.wait()


def land_call(values):
    return pl.pallas_call(
        land_kernel,
        name="land_outputs",
        out_shape=tuple(jax.ShapeDtypeStruct(v.shape, v.dtype) for v in values),
        in_specs=[pl.BlockSpec(memory_space=pltpu.VMEM)] * 4,
        out_specs=(pl.BlockSpec(memory_space=pltpu.HBM),) * 4,
        scratch_shapes=[pltpu.SemaphoreType.DMA((4,))],
        compiler_params=pltpu.CompilerParams(vmem_limit_bytes=4 * 1024 * 1024),
    )(*values)


def on_device(
    hidden, outgrad, row_expert, counts, learner_map, rollout_map, master, moment1, moment2
):
    return land_call(
        step_call(
            hidden[0], outgrad[0], row_expert, counts, learner_map, rollout_map,
            master, moment1, moment2,
        )
    )


def solution(mesh):
    return jax.shard_map(
        on_device,
        mesh=mesh,
        in_specs=(
            P("expert", "dp", None),
            P("expert", "dp", None),
            P("expert", "dp"),
            P("expert", "dp"),
            P(),
            P(),
            P("dp", "expert"),
            P("dp", "expert"),
            P("dp", "expert"),
        ),
        out_specs=(P("dp", "expert"),) * 4,
        check_vma=False,
    )
```

```python
import jax
import jax.numpy as jnp
from jax import lax
from jax.experimental import pallas as pl
from jax.experimental.pallas import tpu as pltpu
from jax.sharding import PartitionSpec as P

MESH = pl.DeviceIdType.MESH
FF = 14336
D = 4096
COLS = 1792
UNIT = 112
GROUPS = 16
HALF_UNITS = FF // UNIT
TOK = 128
CHUNKS = 4
CROWS = TOK // CHUNKS
WIDTH = 256
TILE = 256
PARTS = 2
DROWS = WIDTH // PARTS
FOLD = 16
PACKED = DROWS - FOLD
LANES = 128

beta_one = 0.9
beta_two = 0.95
learn_rate = 0.01
decay_rate = 0.1
epsilon = 1e-08
step_count = 100.0


def dp_of(x, plane, core):
    return (lax.rem(x + 4, 4) * 2 + plane) * 2 + core


def step_kernel(
    hid_ref, og_ref, rexp_ref, lrow_ref, rrow_ref, count_ref,
    master_ref, mom1_ref, mom2_ref,
    new_master, new_mom1, new_mom2, out_ref,
    hid, og, rexp, lrow, rrow, lsm_ref, rsm_ref, master, mom1, mom2, abuf, bbuf, lhs_t, grad,
    index_v, index, value, packed, sends, recv_0, recv_1,
    load_sem, a_send, a_recv, z_send, z_recv, x_send, x_recv, o_send, o_recv, s_send, s_recv,
    e_send, e_recv,
):
    recvs = (recv_0, recv_1)
    dp = lax.axis_index("dp")
    ex = lax.axis_index("expert")
    core = lax.rem(dp, 2)
    plane = lax.rem(dp // 2, 2)
    x = dp // 4
    planes = (plane, 1 - plane)

    barrier = pltpu.get_barrier_semaphore()
    for k in range(1, 16):
        pl.semaphore_signal(barrier, inc=1, device_id=(lax.rem(dp + k, 16), ex), device_id_type=MESH)
    for k in range(1, 16):
        pl.semaphore_signal(barrier, inc=1, device_id=(dp, lax.rem(ex + k, 16)), device_id_type=MESH)
    loads = [
        pltpu.make_async_copy(src, dst, load_sem.at[i])
        for i, (src, dst) in enumerate(
            (
                (lrow_ref, lsm_ref), (rrow_ref, rsm_ref), (hid_ref, hid), (rexp_ref, rexp), (og_ref, og),
                (mom1_ref, mom1), (mom2_ref, mom2), (master_ref, master),
                (lrow_ref, lrow), (rrow_ref, rrow),
            )
        )
    ]
    for load in loads:
        load.start()

    for load in loads[:2]:
        load.wait()
    lane = lax.broadcasted_iota(jnp.int32, (8, COLS), 1)
    unit_of = jnp.zeros((8, COLS), jnp.int32)
    for u in range(GROUPS):
        belongs = (lane >= u * UNIT) & (lane < (u + 1) * UNIT)
        unit_of = jnp.where(belongs, lsm_ref[0, ex * GROUPS + u], unit_of)
    expert_of = jnp.where(unit_of >= HALF_UNITS, 1, 0)[0:1, :]
    rows = lax.broadcasted_iota(jnp.int32, (TOK, TOK), 0)
    cols = lax.broadcasted_iota(jnp.int32, (TOK, TOK), 1)
    for load in loads[2:4]:
        load.wait()
    row_expert = jnp.sum(jnp.where(rows == cols, rexp[...], 0), axis=1, keepdims=True)
    live = lax.broadcasted_iota(jnp.int32, (TOK, 1), 0) < count_ref[0, 0]
    row_key = jnp.where(live, row_expert, -1)
    for j in range(CHUNKS):
        key = row_key[j * CROWS : (j + 1) * CROWS]
        kept = key == expert_of
        block = hid[j * CROWS : (j + 1) * CROWS, :].astype(jnp.float32)
        bbuf[plane, j, x * 2 + core] = jnp.where(kept, block, 0.0).astype(jnp.bfloat16)
    loads[4].wait()
    pl.semaphore_wait(barrier, 30)

    started = []

    def send(src, dst, ssem, rsem, to):
        copy = pltpu.make_async_remote_copy(
            src_ref=src, dst_ref=dst, send_sem=ssem, recv_sem=rsem,
            device_id=to, device_id_type=MESH,
        )
        copy.start()
        started.append(copy)

    def arrived(ref, rsem):
        pltpu.make_async_copy(ref, ref, rsem).wait()

    def a_columns(k, other):
        return pl.ds(pl.multiple_of(other * WIDTH + k * DROWS, DROWS), DROWS)

    def send_a(k, other):
        cut = og.at[:, :, a_columns(k, other)]
        slot_a = abuf.at[k, plane, :, x * 2 + core]
        send(cut, slot_a, a_send.at[k, other], a_recv.at[k, dp], (other, ex))

    def a_across(k):
        for dx in (0, 1, 3, 2):
            for dc in range(2):
                send_a(k, dp_of(x + dx, 1 - plane, lax.rem(core + dc, 2)))

    def a_within(k):
        for dx in (1, 3, 2, 0):
            for dc in range(2):
                if (dx, dc) != (0, 0):
                    send_a(k, dp_of(x + dx, plane, lax.rem(core + dc, 2)))

    def slot(p, j, dx, c):
        return bbuf.at[planes[p], j, lax.rem(x + dx + 4, 4) * 2 + c]

    def peer(dx, c):
        return (dp_of(x + dx, plane, c), ex)

    def center(p, j):
        me = slot(p, j, 0, core)
        send(me, me, x_send.at[p, j, 0], x_recv.at[p, j, 0], peer(1, core))
        send(me, me, x_send.at[p, j, 1], x_recv.at[p, j, 1], peer(-1, core))
        send(me, me, s_send.at[p, j, 0], s_recv.at[p, j, 0], peer(0, 1 - core))

    def z_out(j):
        me = slot(0, j, 0, core)
        send(me, me, z_send.at[j], z_recv.at[j], (dp_of(x, 1 - plane, core), ex))

    def z_in(j):
        arrived(slot(1, j, 0, core), z_recv.at[j])
        center(1, j)

    def sides(p, j):
        left = slot(p, j, -1, core)
        arrived(left, x_recv.at[p, j, 0])
        first = left.at[pl.ds(0, CROWS // 2)]
        send(first, first, o_send.at[p, j, 0], o_recv.at[p, j, 0], peer(1, core))
        send(left, left, s_send.at[p, j, 1], s_recv.at[p, j, 1], peer(0, 1 - core))
        right = slot(p, j, 1, core)
        arrived(right, x_recv.at[p, j, 1])
        second = right.at[pl.ds(CROWS // 2, CROWS // 2)]
        send(second, second, o_send.at[p, j, 1], o_recv.at[p, j, 1], peer(-1, core))
        send(right, right, s_send.at[p, j, 2], s_recv.at[p, j, 2], peer(0, 1 - core))

    def opposite(p, j):
        far = slot(p, j, 2, core)
        arrived(far.at[pl.ds(0, CROWS // 2)], o_recv.at[p, j, 0])
        arrived(far.at[pl.ds(CROWS // 2, CROWS // 2)], o_recv.at[p, j, 1])
        send(far, far, s_send.at[p, j, 3], s_recv.at[p, j, 3], peer(0, 1 - core))

    def wait_a(k, p):
        for dx in range(4):
            for dc in range(2):
                if (p, dx, dc) == (0, 0, 0):
                    continue
                c = lax.rem(core + dc, 2)
                src = dp_of(x + dx, planes[p], c)
                arrived(abuf.at[k, planes[p], :, lax.rem(x + dx, 4) * 2 + c], a_recv.at[k, src])

    def wait_sibling(p):
        for j in range(CHUNKS):
            for i, dx in enumerate((0, -1, 1, 2)):
                arrived(slot(p, j, dx, 1 - core), s_recv.at[p, j, i])

    def multiply(k, p, lo=0, hi=CHUNKS):
        depth = (hi - lo) * 8 * CROWS
        lhs_t[:, :depth] = jnp.transpose(abuf[k, planes[p], lo:hi].reshape(depth, DROWS))

        def tile(t, carry):
            at = pl.ds(pl.multiple_of(t * TILE, TILE), TILE)
            rhs = bbuf[planes[p], lo:hi, :, :, at].reshape(depth, TILE)
            part = jnp.dot(lhs_t[:, :depth], rhs, preferred_element_type=jnp.float32)
            if p == 0 and lo == 0:
                grad[:, at] = part
            else:
                grad[:, at] += part
            return carry

        lax.fori_loop(0, COLS // TILE, tile, 0, unroll=True)

    bias_one = 1.0 - beta_one**step_count
    bias_two = 1.0 - beta_two**step_count

    def update(k):
        def piece(i, carry):
            r = pl.multiple_of(lax.rem(i, DROWS // 32) * 32, 32)
            at = pl.ds(pl.multiple_of((i // (DROWS // 32)) * TILE, TILE), TILE)
            here = (pl.ds(k * DROWS + r, 32), at)
            g = grad[pl.ds(r, 32), at]
            m1 = beta_one * mom1[here] + (1.0 - beta_one) * g
            m2 = beta_two * mom2[here] + (1.0 - beta_two) * g * g
            w = master[here]
            step = m1 * (1.0 / bias_one) / (jnp.sqrt(m2 * (1.0 / bias_two)) + epsilon)
            w = w - learn_rate * (step + decay_rate * w)
            new_mom1[here] = m1
            new_mom2[here] = m2
            new_master[here] = w
            value[pl.ds(r, 32), at] = w.astype(jnp.bfloat16)
            return carry

        lax.fori_loop(0, (DROWS // 32) * (COLS // TILE), piece, 0, unroll=4)

    lane_fold = lax.broadcasted_iota(jnp.int32, (FOLD, LANES), 1)
    lane_all = lax.broadcasted_iota(jnp.int32, (DROWS, LANES), 1)

    def shifted(val, by):
        by = by % LANES
        return val if by == 0 else pltpu.roll(val, by, 1)

    def pack():
        for u in range(GROUPS):
            block, off = divmod(u * UNIT, LANES)
            one = shifted(value[:, block * LANES : (block + 1) * LANES], -off)
            if off + UNIT > LANES:
                two = shifted(value[:, (block + 1) * LANES : (block + 2) * LANES], -off)
                one = jnp.where(lane_all < LANES - off, one, two)
            last = one[PACKED:]
            for g in range(PACKED // FOLD):
                extra = shifted(last, UNIT - 16 * g)
                mine = one[g * FOLD : (g + 1) * FOLD]
                packed[u, g * FOLD : (g + 1) * FOLD, :] = jnp.where(lane_fold < UNIT, mine, extra)

    def spread(k):
        def to_slot(i, carry):
            sends[k, i] = packed[index[0, lax.rem(ex + i, GROUPS)]]
            return carry

        lax.fori_loop(0, GROUPS, to_slot, 0)
        for i in range(1, GROUPS):
            to = lax.rem(ex + i, GROUPS)
            send(sends.at[k, i], recvs[k].at[ex], e_send.at[k, i], e_recv.at[k, i], (dp, to))
        recvs[k][ex] = sends[k, 0]

    def collect(k):
        for i in range(1, GROUPS):
            arrived(recvs[k].at[lax.rem(ex - i + GROUPS, GROUPS)], e_recv.at[k, i])

        def unfolded(p):
            data = recvs[k][index[1, p]]
            tail = jnp.zeros((FOLD, LANES), data.dtype)
            for g in range(PACKED // FOLD):
                moved = shifted(data[g * FOLD : (g + 1) * FOLD], 16 * g - UNIT)
                tail = jnp.where((lane_fold >= 16 * g) & (lane_fold < 16 * g + 16), moved, tail)
            return jnp.concatenate([data, tail], axis=0)

        held = unfolded(0)
        pos = 0
        for q in range(COLS // LANES):
            off = q * LANES - pos * UNIT
            nxt = unfolded(pos + 1)
            a = shifted(held, -off)
            b = shifted(nxt, UNIT - off)
            joined = jnp.where(lane_all < UNIT - off, a, b)
            out_ref[k * DROWS : (k + 1) * DROWS, q * LANES : (q + 1) * LANES] = joined
            pos += 1
            held = nxt
            if (q + 1) * LANES - pos * UNIT == UNIT and pos + 1 < GROUPS:
                pos += 1
                held = unfolded(pos)

    for j in range(CHUNKS):
        z_out(j)
        center(0, j)
    a_within(0)
    for k in range(PARTS):
        for j in range(CHUNKS):
            abuf[k, plane, j, x * 2 + core] = og[j, :, a_columns(k, dp)]

    for load in loads[8:]:
        load.wait()
    wide = lax.broadcasted_iota(jnp.int32, (GROUPS, 256), 1) // GROUPS
    high = lax.broadcasted_iota(jnp.int32, (GROUPS, 1), 0)
    have = jnp.zeros((GROUPS, 1), jnp.int32)
    wanted = jnp.zeros((GROUPS, 1), jnp.int32)
    for u in range(GROUPS):
        have = jnp.where(high == u, lsm_ref[0, ex * GROUPS + u], have)
        wanted = jnp.where(high == u, rsm_ref[0, ex * GROUPS + u], wanted)
    target = jnp.max(jnp.where(rrow[...] == have, wide, 0), axis=1, keepdims=True)
    source = jnp.max(jnp.where(lrow[...] == wanted, wide, 0), axis=1, keepdims=True)
    low = lax.broadcasted_iota(jnp.int32, (GROUPS, 128), 1)
    high = lax.broadcasted_iota(jnp.int32, (GROUPS, 128), 0)
    index_v[0:1, :] = jnp.max(jnp.where(target == low, high, 0), axis=0, keepdims=True)
    index_v[1:2, :] = jnp.max(jnp.where(high == low, source, 0), axis=0, keepdims=True)
    to_scalar = pltpu.make_async_copy(index_v, index, load_sem.at[10])

    sides(0, 0)
    sides(0, 1)
    to_scalar.start()
    z_in(0)
    sides(0, 2)
    sides(0, 3)
    z_in(1)
    a_across(0)
    opposite(0, 0)
    opposite(0, 1)
    z_in(2)
    opposite(0, 2)
    opposite(0, 3)
    sides(1, 0)
    z_in(3)
    a_across(1)
    a_within(1)
    to_scalar.wait()
    for load in loads[5:8]:
        load.wait()
    sides(1, 1)
    wait_sibling(0)
    wait_a(0, 0)
    multiply(0, 0, 0, 2)
    sides(1, 2)
    multiply(0, 0, 2, 4)
    sides(1, 3)
    for j in range(CHUNKS):
        opposite(1, j)
    wait_sibling(1)
    wait_a(0, 1)
    multiply(0, 1)
    update(0)
    pack()
    spread(0)
    wait_a(1, 0)
    multiply(1, 0)
    wait_a(1, 1)
    multiply(1, 1)
    update(1)
    pack()
    spread(1)
    collect(0)
    collect(1)
    for copy in started:
        copy.wait_send()


def step_call(hidden, outgrad, row_expert, counts, learner_map, rollout_map, master, mom1, mom2):
    vmem = pl.BlockSpec(memory_space=pltpu.VMEM)
    hbm = pl.BlockSpec(memory_space=pltpu.HBM)
    dma = pltpu.SemaphoreType.DMA
    state = pltpu.VMEM((WIDTH, COLS), jnp.float32)

    def far(value):
        return pltpu.with_memory_space_constraint(value, pltpu.HBM)

    return pl.pallas_call(
        step_kernel,
        name="grad_update_spread",
        out_shape=(state, state, state, pltpu.VMEM((WIDTH, COLS), jnp.bfloat16)),
        in_specs=[hbm] * 5 + [pl.BlockSpec(memory_space=pltpu.SMEM)] + [hbm] * 3,
        out_specs=(vmem, vmem, vmem, vmem),
        scratch_shapes=[
            pltpu.VMEM((TOK, COLS), jnp.bfloat16),
            pltpu.VMEM((CHUNKS, CROWS, D), jnp.bfloat16),
            pltpu.VMEM((1, TOK), jnp.int32),
            pltpu.VMEM((1, 256), jnp.int32),
            pltpu.VMEM((1, 256), jnp.int32),
            pltpu.SMEM((1, 256), jnp.int32),
            pltpu.SMEM((1, 256), jnp.int32),
            pltpu.VMEM((WIDTH, COLS), jnp.float32),
            pltpu.VMEM((WIDTH, COLS), jnp.float32),
            pltpu.VMEM((WIDTH, COLS), jnp.float32),
            pltpu.VMEM((PARTS, 2, CHUNKS, 8, CROWS, DROWS), jnp.bfloat16),
            pltpu.VMEM((2, CHUNKS, 8, CROWS, COLS), jnp.bfloat16),
            pltpu.VMEM((DROWS, 8 * TOK), jnp.bfloat16),
            pltpu.VMEM((DROWS, COLS), jnp.float32),
            pltpu.VMEM((2, 128), jnp.int32),
            pltpu.SMEM((2, 128), jnp.int32),
            pltpu.VMEM((DROWS, COLS), jnp.bfloat16),
            pltpu.VMEM((GROUPS, PACKED, LANES), jnp.bfloat16),
            pltpu.VMEM((PARTS, GROUPS, PACKED, LANES), jnp.bfloat16),
            pltpu.VMEM((GROUPS, PACKED, LANES), jnp.bfloat16),
            pltpu.VMEM((GROUPS, PACKED, LANES), jnp.bfloat16),
            dma((11,)),
            dma((PARTS, 16)), dma((PARTS, 16)),
            dma((CHUNKS,)), dma((CHUNKS,)),
            dma((2, CHUNKS, 2)), dma((2, CHUNKS, 2)),
            dma((2, CHUNKS, 2)), dma((2, CHUNKS, 2)),
            dma((2, CHUNKS, 4)), dma((2, CHUNKS, 4)),
            dma((PARTS, GROUPS)), dma((PARTS, GROUPS)),
        ],
        compiler_params=pltpu.CompilerParams(
            collective_id=0, has_side_effects=True, vmem_limit_bytes=40 * 1024 * 1024
        ),
    )(
        far(hidden),
        far(outgrad.reshape(CHUNKS, CROWS, D)),
        far(row_expert),
        far(learner_map.reshape(1, 256)),
        far(rollout_map.reshape(1, 256)),
        counts,
        far(master),
        far(mom1),
        far(mom2),
    )


def land_kernel(*refs):
    ins, outs, sem = refs[:4], refs[4:8], refs[8]
    copies = [pltpu.make_async_copy(a, b, sem.at[i]) for i, (a, b) in enumerate(zip(ins, outs))]
    for copy in copies:
        copy.start()
    for copy in copies:
        copy.wait()


def land_call(values):
    return pl.pallas_call(
        land_kernel,
        name="land_outputs",
        out_shape=tuple(jax.ShapeDtypeStruct(v.shape, v.dtype) for v in values),
        in_specs=[pl.BlockSpec(memory_space=pltpu.VMEM)] * 4,
        out_specs=(pl.BlockSpec(memory_space=pltpu.HBM),) * 4,
        scratch_shapes=[pltpu.SemaphoreType.DMA((4,))],
        compiler_params=pltpu.CompilerParams(vmem_limit_bytes=4 * 1024 * 1024),
    )(*values)


def on_device(
    hidden, outgrad, row_expert, counts, learner_map, rollout_map, master, moment1, moment2
):
    return land_call(
        step_call(
            hidden[0], outgrad[0], row_expert, counts, learner_map, rollout_map,
            master, moment1, moment2,
        )
    )


def solution(mesh):
    return jax.shard_map(
        on_device,
        mesh=mesh,
        in_specs=(
            P("expert", "dp", None),
            P("expert", "dp", None),
            P("expert", "dp"),
            P("expert", "dp"),
            P(),
            P(),
            P("dp", "expert"),
            P("dp", "expert"),
            P("dp", "expert"),
        ),
        out_specs=(P("dp", "expert"),) * 4,
        check_vma=False,
    )
```

```python
import jax
import jax.numpy as jnp
from jax import lax
from jax.experimental import pallas as pl
from jax.experimental.pallas import tpu as pltpu
from jax.sharding import PartitionSpec as P

MESH = pl.DeviceIdType.MESH
FF = 14336
D = 4096
COLS = 1792
UNIT = 112
GROUPS = 16
HALF_UNITS = FF // UNIT
TOK = 128
CHUNKS = 4
CROWS = TOK // CHUNKS
WIDTH = 256
TILE = 256
PARTS = 2
DROWS = WIDTH // PARTS
FOLD = 16
PACKED = DROWS - FOLD
LANES = 128

beta_one = 0.9
beta_two = 0.95
learn_rate = 0.01
decay_rate = 0.1
epsilon = 1e-08
step_count = 100.0


def dp_of(x, plane, core):
    return (lax.rem(x + 4, 4) * 2 + plane) * 2 + core


def step_kernel(
    hid_ref, og_ref, rexp_ref, lrow_ref, rrow_ref, count_ref,
    master_ref, mom1_ref, mom2_ref,
    new_master, new_mom1, new_mom2, out_ref,
    hid, og, rexp, lrow, rrow, lsm_ref, rsm_ref, master, mom1, mom2, abuf, bbuf, lhs_t, grad,
    index_v, index, value, packed, sends, recv_0, recv_1,
    load_sem, a_send, a_recv, z_send, z_recv, x_send, x_recv, o_send, o_recv, s_send, s_recv,
    e_send, e_recv,
):
    recvs = (recv_0, recv_1)
    dp = lax.axis_index("dp")
    ex = lax.axis_index("expert")
    core = lax.rem(dp, 2)
    plane = lax.rem(dp // 2, 2)
    x = dp // 4
    planes = (plane, 1 - plane)

    barrier = pltpu.get_barrier_semaphore()
    for k in range(1, 16):
        pl.semaphore_signal(barrier, inc=1, device_id=(lax.rem(dp + k, 16), ex), device_id_type=MESH)
    for k in range(1, 16):
        pl.semaphore_signal(barrier, inc=1, device_id=(dp, lax.rem(ex + k, 16)), device_id_type=MESH)
    loads = [
        pltpu.make_async_copy(src, dst, load_sem.at[i])
        for i, (src, dst) in enumerate(
            (
                (lrow_ref, lsm_ref), (rrow_ref, rsm_ref), (hid_ref, hid), (rexp_ref, rexp), (og_ref, og),
                (mom1_ref, mom1), (mom2_ref, mom2), (master_ref, master),
                (lrow_ref, lrow), (rrow_ref, rrow),
            )
        )
    ]
    for load in loads:
        load.start()

    for load in loads[:2]:
        load.wait()
    lane = lax.broadcasted_iota(jnp.int32, (8, COLS), 1)
    unit_of = jnp.zeros((8, COLS), jnp.int32)
    for u in range(GROUPS):
        belongs = (lane >= u * UNIT) & (lane < (u + 1) * UNIT)
        unit_of = jnp.where(belongs, lsm_ref[0, ex * GROUPS + u], unit_of)
    expert_of = jnp.where(unit_of >= HALF_UNITS, 1, 0)[0:1, :]
    rows = lax.broadcasted_iota(jnp.int32, (TOK, TOK), 0)
    cols = lax.broadcasted_iota(jnp.int32, (TOK, TOK), 1)
    for load in loads[2:4]:
        load.wait()
    row_expert = jnp.sum(jnp.where(rows == cols, rexp[...], 0), axis=1, keepdims=True)
    live = lax.broadcasted_iota(jnp.int32, (TOK, 1), 0) < count_ref[0, 0]
    row_key = jnp.where(live, row_expert, -1)
    for j in range(CHUNKS):
        key = row_key[j * CROWS : (j + 1) * CROWS]
        kept = key == expert_of
        block = hid[j * CROWS : (j + 1) * CROWS, :].astype(jnp.float32)
        bbuf[plane, j, x * 2 + core] = jnp.where(kept, block, 0.0).astype(jnp.bfloat16)
    loads[4].wait()
    pl.semaphore_wait(barrier, 30)

    started = []

    def send(src, dst, ssem, rsem, to):
        copy = pltpu.make_async_remote_copy(
            src_ref=src, dst_ref=dst, send_sem=ssem, recv_sem=rsem,
            device_id=to, device_id_type=MESH,
        )
        copy.start()
        started.append(copy)

    def arrived(ref, rsem):
        pltpu.make_async_copy(ref, ref, rsem).wait()

    def a_columns(k, other):
        return pl.ds(pl.multiple_of(other * WIDTH + k * DROWS, DROWS), DROWS)

    def send_a(k, other):
        cut = og.at[:, :, a_columns(k, other)]
        slot_a = abuf.at[k, plane, :, x * 2 + core]
        send(cut, slot_a, a_send.at[k, other], a_recv.at[k, dp], (other, ex))

    def a_across(k):
        for dx in (0, 1, 3, 2):
            for dc in range(2):
                send_a(k, dp_of(x + dx, 1 - plane, lax.rem(core + dc, 2)))

    def a_within(k):
        for dx in (1, 3, 2, 0):
            for dc in range(2):
                if (dx, dc) != (0, 0):
                    send_a(k, dp_of(x + dx, plane, lax.rem(core + dc, 2)))

    def slot(p, j, dx, c):
        return bbuf.at[planes[p], j, lax.rem(x + dx + 4, 4) * 2 + c]

    def peer(dx, c):
        return (dp_of(x + dx, plane, c), ex)

    def center(p, j):
        me = slot(p, j, 0, core)
        send(me, me, x_send.at[p, j, 0], x_recv.at[p, j, 0], peer(1, core))
        send(me, me, x_send.at[p, j, 1], x_recv.at[p, j, 1], peer(-1, core))
        send(me, me, s_send.at[p, j, 0], s_recv.at[p, j, 0], peer(0, 1 - core))

    def z_out(j):
        me = slot(0, j, 0, core)
        send(me, me, z_send.at[j], z_recv.at[j], (dp_of(x, 1 - plane, core), ex))

    def z_in(j):
        arrived(slot(1, j, 0, core), z_recv.at[j])
        center(1, j)

    def sides(p, j):
        left = slot(p, j, -1, core)
        arrived(left, x_recv.at[p, j, 0])
        first = left.at[pl.ds(0, CROWS // 2)]
        send(first, first, o_send.at[p, j, 0], o_recv.at[p, j, 0], peer(1, core))
        send(left, left, s_send.at[p, j, 1], s_recv.at[p, j, 1], peer(0, 1 - core))
        right = slot(p, j, 1, core)
        arrived(right, x_recv.at[p, j, 1])
        second = right.at[pl.ds(CROWS // 2, CROWS // 2)]
        send(second, second, o_send.at[p, j, 1], o_recv.at[p, j, 1], peer(-1, core))
        send(right, right, s_send.at[p, j, 2], s_recv.at[p, j, 2], peer(0, 1 - core))

    def opposite(p, j):
        far = slot(p, j, 2, core)
        arrived(far.at[pl.ds(0, CROWS // 2)], o_recv.at[p, j, 0])
        arrived(far.at[pl.ds(CROWS // 2, CROWS // 2)], o_recv.at[p, j, 1])
        send(far, far, s_send.at[p, j, 3], s_recv.at[p, j, 3], peer(0, 1 - core))

    def wait_a(k, p):
        for dx in range(4):
            for dc in range(2):
                if (p, dx, dc) == (0, 0, 0):
                    continue
                c = lax.rem(core + dc, 2)
                src = dp_of(x + dx, planes[p], c)
                arrived(abuf.at[k, planes[p], :, lax.rem(x + dx, 4) * 2 + c], a_recv.at[k, src])

    def wait_sibling(p):
        for j in range(CHUNKS):
            for i, dx in enumerate((0, -1, 1, 2)):
                arrived(slot(p, j, dx, 1 - core), s_recv.at[p, j, i])

    def multiply(k, p, lo=0, hi=CHUNKS):
        depth = (hi - lo) * 8 * CROWS
        lhs_t[:, :depth] = jnp.transpose(abuf[k, planes[p], lo:hi].reshape(depth, DROWS))

        def tile(t, carry):
            at = pl.ds(pl.multiple_of(t * TILE, TILE), TILE)
            rhs = bbuf[planes[p], lo:hi, :, :, at].reshape(depth, TILE)
            part = jnp.dot(lhs_t[:, :depth], rhs, preferred_element_type=jnp.float32)
            if p == 0 and lo == 0:
                grad[:, at] = part
            else:
                grad[:, at] += part
            return carry

        lax.fori_loop(0, COLS // TILE, tile, 0, unroll=True)

    bias_one = 1.0 - beta_one**step_count
    bias_two = 1.0 - beta_two**step_count

    def update(k):
        def piece(i, carry):
            r = pl.multiple_of(lax.rem(i, DROWS // 32) * 32, 32)
            at = pl.ds(pl.multiple_of((i // (DROWS // 32)) * TILE, TILE), TILE)
            here = (pl.ds(k * DROWS + r, 32), at)
            g = grad[pl.ds(r, 32), at]
            m1 = beta_one * mom1[here] + (1.0 - beta_one) * g
            m2 = beta_two * mom2[here] + (1.0 - beta_two) * g * g
            w = master[here]
            step = m1 * (1.0 / bias_one) / (jnp.sqrt(m2 * (1.0 / bias_two)) + epsilon)
            w = w - learn_rate * (step + decay_rate * w)
            new_mom1[here] = m1
            new_mom2[here] = m2
            new_master[here] = w
            value[pl.ds(r, 32), at] = w.astype(jnp.bfloat16)
            return carry

        lax.fori_loop(0, (DROWS // 32) * (COLS // TILE), piece, 0, unroll=4)

    lane_fold = lax.broadcasted_iota(jnp.int32, (FOLD, LANES), 1)
    lane_all = lax.broadcasted_iota(jnp.int32, (DROWS, LANES), 1)

    def shifted(val, by):
        by = by % LANES
        return val if by == 0 else pltpu.roll(val, by, 1)

    def pack():
        for u in range(GROUPS):
            at = u * UNIT
            packed[u, :, :UNIT] = value[:PACKED, at : at + UNIT]
            for g in range(PACKED // FOLD):
                extra = value[PACKED:, at + 16 * g : at + 16 * g + 16]
                packed[u, g * FOLD : (g + 1) * FOLD, UNIT:] = extra

    def spread(k):
        def to_slot(i, carry):
            sends[k, i] = packed[index[0, lax.rem(ex + i, GROUPS)]]
            return carry

        lax.fori_loop(0, GROUPS, to_slot, 0)
        for i in range(1, GROUPS):
            to = lax.rem(ex + i, GROUPS)
            send(sends.at[k, i], recvs[k].at[ex], e_send.at[k, i], e_recv.at[k, i], (dp, to))
        recvs[k][ex] = sends[k, 0]

    def collect(k):
        for i in range(1, GROUPS):
            arrived(recvs[k].at[lax.rem(ex - i + GROUPS, GROUPS)], e_recv.at[k, i])

        def unfolded(p):
            data = recvs[k][index[1, p]]
            tail = jnp.zeros((FOLD, LANES), data.dtype)
            for g in range(PACKED // FOLD):
                moved = shifted(data[g * FOLD : (g + 1) * FOLD], 16 * g - UNIT)
                tail = jnp.where((lane_fold >= 16 * g) & (lane_fold < 16 * g + 16), moved, tail)
            return jnp.concatenate([data, tail], axis=0)

        held = unfolded(0)
        pos = 0
        for q in range(COLS // LANES):
            off = q * LANES - pos * UNIT
            nxt = unfolded(pos + 1)
            a = shifted(held, -off)
            b = shifted(nxt, UNIT - off)
            joined = jnp.where(lane_all < UNIT - off, a, b)
            out_ref[k * DROWS : (k + 1) * DROWS, q * LANES : (q + 1) * LANES] = joined
            pos += 1
            held = nxt
            if (q + 1) * LANES - pos * UNIT == UNIT and pos + 1 < GROUPS:
                pos += 1
                held = unfolded(pos)

    for j in range(CHUNKS):
        z_out(j)
        center(0, j)
    a_within(0)
    for k in range(PARTS):
        for j in range(CHUNKS):
            abuf[k, plane, j, x * 2 + core] = og[j, :, a_columns(k, dp)]

    for load in loads[8:]:
        load.wait()
    wide = lax.broadcasted_iota(jnp.int32, (GROUPS, 256), 1) // GROUPS
    high = lax.broadcasted_iota(jnp.int32, (GROUPS, 1), 0)
    have = jnp.zeros((GROUPS, 1), jnp.int32)
    wanted = jnp.zeros((GROUPS, 1), jnp.int32)
    for u in range(GROUPS):
        have = jnp.where(high == u, lsm_ref[0, ex * GROUPS + u], have)
        wanted = jnp.where(high == u, rsm_ref[0, ex * GROUPS + u], wanted)
    target = jnp.max(jnp.where(rrow[...] == have, wide, 0), axis=1, keepdims=True)
    source = jnp.max(jnp.where(lrow[...] == wanted, wide, 0), axis=1, keepdims=True)
    low = lax.broadcasted_iota(jnp.int32, (GROUPS, 128), 1)
    high = lax.broadcasted_iota(jnp.int32, (GROUPS, 128), 0)
    index_v[0:1, :] = jnp.max(jnp.where(target == low, high, 0), axis=0, keepdims=True)
    index_v[1:2, :] = jnp.max(jnp.where(high == low, source, 0), axis=0, keepdims=True)
    to_scalar = pltpu.make_async_copy(index_v, index, load_sem.at[10])

    sides(0, 0)
    sides(0, 1)
    to_scalar.start()
    z_in(0)
    sides(0, 2)
    sides(0, 3)
    z_in(1)
    a_across(0)
    opposite(0, 0)
    opposite(0, 1)
    z_in(2)
    opposite(0, 2)
    opposite(0, 3)
    sides(1, 0)
    z_in(3)
    a_across(1)
    a_within(1)
    to_scalar.wait()
    for load in loads[5:8]:
        load.wait()
    sides(1, 1)
    wait_sibling(0)
    wait_a(0, 0)
    multiply(0, 0, 0, 2)
    sides(1, 2)
    multiply(0, 0, 2, 4)
    sides(1, 3)
    for j in range(CHUNKS):
        opposite(1, j)
    wait_sibling(1)
    wait_a(0, 1)
    multiply(0, 1)
    update(0)
    pack()
    spread(0)
    wait_a(1, 0)
    multiply(1, 0)
    wait_a(1, 1)
    multiply(1, 1)
    update(1)
    pack()
    spread(1)
    for copy in started[: 1 - GROUPS]:
        copy.wait_send()
    collect(0)
    for copy in started[1 - GROUPS :]:
        copy.wait_send()
    collect(1)


def step_call(hidden, outgrad, row_expert, counts, learner_map, rollout_map, master, mom1, mom2):
    vmem = pl.BlockSpec(memory_space=pltpu.VMEM)
    hbm = pl.BlockSpec(memory_space=pltpu.HBM)
    dma = pltpu.SemaphoreType.DMA
    state = pltpu.VMEM((WIDTH, COLS), jnp.float32)

    def far(value):
        return pltpu.with_memory_space_constraint(value, pltpu.HBM)

    return pl.pallas_call(
        step_kernel,
        name="grad_update_spread",
        out_shape=(state, state, state, pltpu.VMEM((WIDTH, COLS), jnp.bfloat16)),
        in_specs=[hbm] * 5 + [pl.BlockSpec(memory_space=pltpu.SMEM)] + [hbm] * 3,
        out_specs=(vmem, vmem, vmem, vmem),
        scratch_shapes=[
            pltpu.VMEM((TOK, COLS), jnp.bfloat16),
            pltpu.VMEM((CHUNKS, CROWS, D), jnp.bfloat16),
            pltpu.VMEM((1, TOK), jnp.int32),
            pltpu.VMEM((1, 256), jnp.int32),
            pltpu.VMEM((1, 256), jnp.int32),
            pltpu.SMEM((1, 256), jnp.int32),
            pltpu.SMEM((1, 256), jnp.int32),
            pltpu.VMEM((WIDTH, COLS), jnp.float32),
            pltpu.VMEM((WIDTH, COLS), jnp.float32),
            pltpu.VMEM((WIDTH, COLS), jnp.float32),
            pltpu.VMEM((PARTS, 2, CHUNKS, 8, CROWS, DROWS), jnp.bfloat16),
            pltpu.VMEM((2, CHUNKS, 8, CROWS, COLS), jnp.bfloat16),
            pltpu.VMEM((DROWS, 8 * TOK), jnp.bfloat16),
            pltpu.VMEM((DROWS, COLS), jnp.float32),
            pltpu.VMEM((2, 128), jnp.int32),
            pltpu.SMEM((2, 128), jnp.int32),
            pltpu.VMEM((DROWS, COLS), jnp.bfloat16),
            pltpu.VMEM((GROUPS, PACKED, LANES), jnp.bfloat16),
            pltpu.VMEM((PARTS, GROUPS, PACKED, LANES), jnp.bfloat16),
            pltpu.VMEM((GROUPS, PACKED, LANES), jnp.bfloat16),
            pltpu.VMEM((GROUPS, PACKED, LANES), jnp.bfloat16),
            dma((11,)),
            dma((PARTS, 16)), dma((PARTS, 16)),
            dma((CHUNKS,)), dma((CHUNKS,)),
            dma((2, CHUNKS, 2)), dma((2, CHUNKS, 2)),
            dma((2, CHUNKS, 2)), dma((2, CHUNKS, 2)),
            dma((2, CHUNKS, 4)), dma((2, CHUNKS, 4)),
            dma((PARTS, GROUPS)), dma((PARTS, GROUPS)),
        ],
        compiler_params=pltpu.CompilerParams(
            collective_id=0, has_side_effects=True, vmem_limit_bytes=40 * 1024 * 1024
        ),
    )(
        far(hidden),
        far(outgrad.reshape(CHUNKS, CROWS, D)),
        far(row_expert),
        far(learner_map.reshape(1, 256)),
        far(rollout_map.reshape(1, 256)),
        counts,
        far(master),
        far(mom1),
        far(mom2),
    )


def land_kernel(*refs):
    ins, outs, sem = refs[:4], refs[4:8], refs[8]
    copies = [pltpu.make_async_copy(a, b, sem.at[i]) for i, (a, b) in enumerate(zip(ins, outs))]
    for copy in copies:
        copy.start()
    for copy in copies:
        copy.wait()


def land_call(values):
    return pl.pallas_call(
        land_kernel,
        name="land_outputs",
        out_shape=tuple(jax.ShapeDtypeStruct(v.shape, v.dtype) for v in values),
        in_specs=[pl.BlockSpec(memory_space=pltpu.VMEM)] * 4,
        out_specs=(pl.BlockSpec(memory_space=pltpu.HBM),) * 4,
        scratch_shapes=[pltpu.SemaphoreType.DMA((4,))],
        compiler_params=pltpu.CompilerParams(vmem_limit_bytes=4 * 1024 * 1024),
    )(*values)


def on_device(
    hidden, outgrad, row_expert, counts, learner_map, rollout_map, master, moment1, moment2
):
    return land_call(
        step_call(
            hidden[0], outgrad[0], row_expert, counts, learner_map, rollout_map,
            master, moment1, moment2,
        )
    )


def solution(mesh):
    return jax.shard_map(
        on_device,
        mesh=mesh,
        in_specs=(
            P("expert", "dp", None),
            P("expert", "dp", None),
            P("expert", "dp"),
            P("expert", "dp"),
            P(),
            P(),
            P("dp", "expert"),
            P("dp", "expert"),
            P("dp", "expert"),
        ),
        out_specs=(P("dp", "expert"),) * 4,
        check_vma=False,
    )
```

```python
import jax
import jax.numpy as jnp
from jax import lax
from jax.experimental import pallas as pl
from jax.experimental.pallas import tpu as pltpu
from jax.sharding import PartitionSpec as P

MESH = pl.DeviceIdType.MESH
FF = 14336
D = 4096
COLS = 1792
UNIT = 112
GROUPS = 16
HALF_UNITS = FF // UNIT
TOK = 128
CHUNKS = 4
CROWS = TOK // CHUNKS
WIDTH = 256
TILE = 256
PARTS = 2
DROWS = WIDTH // PARTS
FOLD = 16
PACKED = DROWS - FOLD
LANES = 128

beta_one = 0.9
beta_two = 0.95
learn_rate = 0.01
decay_rate = 0.1
epsilon = 1e-08
step_count = 100.0


def dp_of(x, plane, core):
    return (lax.rem(x + 4, 4) * 2 + plane) * 2 + core


def step_kernel(
    hid_ref, og_ref, rexp_ref, lrow_ref, rrow_ref, count_ref,
    master_ref, mom1_ref, mom2_ref,
    new_master, new_mom1, new_mom2, out_ref,
    hid, og, rexp, lrow, rrow, lsm_ref, rsm_ref, master, mom1, mom2, abuf, bbuf, lhs_t, grad,
    index_v, index, value, packed, sends, recv_0, recv_1,
    load_sem, a_send, a_recv, z_send, z_recv, x_send, x_recv, o_send, o_recv, s_send, s_recv,
    e_send, e_recv,
):
    recvs = (recv_0, recv_1)
    dp = lax.axis_index("dp")
    ex = lax.axis_index("expert")
    core = lax.rem(dp, 2)
    plane = lax.rem(dp // 2, 2)
    x = dp // 4
    planes = (plane, 1 - plane)

    barrier = pltpu.get_barrier_semaphore()
    for k in range(1, 16):
        pl.semaphore_signal(barrier, inc=1, device_id=(lax.rem(dp + k, 16), ex), device_id_type=MESH)
    for k in range(1, 16):
        pl.semaphore_signal(barrier, inc=1, device_id=(dp, lax.rem(ex + k, 16)), device_id_type=MESH)
    loads = [
        pltpu.make_async_copy(src, dst, load_sem.at[i])
        for i, (src, dst) in enumerate(
            (
                (lrow_ref, lsm_ref), (rrow_ref, rsm_ref), (hid_ref, hid), (rexp_ref, rexp), (og_ref, og),
                (mom1_ref, mom1), (mom2_ref, mom2), (master_ref, master),
                (lrow_ref, lrow), (rrow_ref, rrow),
            )
        )
    ]
    for load in loads:
        load.start()

    for load in loads[:2]:
        load.wait()
    lane = lax.broadcasted_iota(jnp.int32, (8, COLS), 1)
    unit_of = jnp.zeros((8, COLS), jnp.int32)
    for u in range(GROUPS):
        belongs = (lane >= u * UNIT) & (lane < (u + 1) * UNIT)
        unit_of = jnp.where(belongs, lsm_ref[0, ex * GROUPS + u], unit_of)
    expert_of = jnp.where(unit_of >= HALF_UNITS, 1, 0)[0:1, :]
    rows = lax.broadcasted_iota(jnp.int32, (TOK, TOK), 0)
    cols = lax.broadcasted_iota(jnp.int32, (TOK, TOK), 1)
    for load in loads[2:4]:
        load.wait()
    row_expert = jnp.sum(jnp.where(rows == cols, rexp[...], 0), axis=1, keepdims=True)
    live = lax.broadcasted_iota(jnp.int32, (TOK, 1), 0) < count_ref[0, 0]
    row_key = jnp.where(live, row_expert, -1)
    for j in range(CHUNKS):
        key = row_key[j * CROWS : (j + 1) * CROWS]
        kept = key == expert_of
        block = hid[j * CROWS : (j + 1) * CROWS, :].astype(jnp.float32)
        bbuf[plane, j, x * 2 + core] = jnp.where(kept, block, 0.0).astype(jnp.bfloat16)
    loads[4].wait()
    pl.semaphore_wait(barrier, 30)

    started = []

    def send(src, dst, ssem, rsem, to):
        copy = pltpu.make_async_remote_copy(
            src_ref=src, dst_ref=dst, send_sem=ssem, recv_sem=rsem,
            device_id=to, device_id_type=MESH,
        )
        copy.start()
        started.append(copy)

    def arrived(ref, rsem):
        pltpu.make_async_copy(ref, ref, rsem).wait()

    def a_columns(k, other):
        return pl.ds(pl.multiple_of(other * WIDTH + k * DROWS, DROWS), DROWS)

    def send_a(k, other):
        cut = og.at[:, :, a_columns(k, other)]
        slot_a = abuf.at[k, plane, :, x * 2 + core]
        send(cut, slot_a, a_send.at[k, other], a_recv.at[k, dp], (other, ex))

    def a_across(k):
        for dx in (0, 1, 3, 2):
            for dc in range(2):
                send_a(k, dp_of(x + dx, 1 - plane, lax.rem(core + dc, 2)))

    def a_within(k):
        for dx in (1, 3, 2, 0):
            for dc in range(2):
                if (dx, dc) != (0, 0):
                    send_a(k, dp_of(x + dx, plane, lax.rem(core + dc, 2)))

    def slot(p, j, dx, c):
        return bbuf.at[planes[p], j, lax.rem(x + dx + 4, 4) * 2 + c]

    def peer(dx, c):
        return (dp_of(x + dx, plane, c), ex)

    def center(p, j):
        me = slot(p, j, 0, core)
        send(me, me, x_send.at[p, j, 0], x_recv.at[p, j, 0], peer(1, core))
        send(me, me, x_send.at[p, j, 1], x_recv.at[p, j, 1], peer(-1, core))
        send(me, me, s_send.at[p, j, 0], s_recv.at[p, j, 0], peer(0, 1 - core))

    def z_out(j):
        me = slot(0, j, 0, core)
        send(me, me, z_send.at[j], z_recv.at[j], (dp_of(x, 1 - plane, core), ex))

    def z_in(j):
        arrived(slot(1, j, 0, core), z_recv.at[j])
        center(1, j)

    def sides(p, j):
        left = slot(p, j, -1, core)
        arrived(left, x_recv.at[p, j, 0])
        first = left.at[pl.ds(0, CROWS // 2)]
        send(first, first, o_send.at[p, j, 0], o_recv.at[p, j, 0], peer(1, core))
        send(left, left, s_send.at[p, j, 1], s_recv.at[p, j, 1], peer(0, 1 - core))
        right = slot(p, j, 1, core)
        arrived(right, x_recv.at[p, j, 1])
        second = right.at[pl.ds(CROWS // 2, CROWS // 2)]
        send(second, second, o_send.at[p, j, 1], o_recv.at[p, j, 1], peer(-1, core))
        send(right, right, s_send.at[p, j, 2], s_recv.at[p, j, 2], peer(0, 1 - core))

    def opposite(p, j):
        far = slot(p, j, 2, core)
        arrived(far.at[pl.ds(0, CROWS // 2)], o_recv.at[p, j, 0])
        arrived(far.at[pl.ds(CROWS // 2, CROWS // 2)], o_recv.at[p, j, 1])
        send(far, far, s_send.at[p, j, 3], s_recv.at[p, j, 3], peer(0, 1 - core))

    def wait_a(k, p):
        for dx in range(4):
            for dc in range(2):
                if (p, dx, dc) == (0, 0, 0):
                    continue
                c = lax.rem(core + dc, 2)
                src = dp_of(x + dx, planes[p], c)
                arrived(abuf.at[k, planes[p], :, lax.rem(x + dx, 4) * 2 + c], a_recv.at[k, src])

    def wait_sibling(p):
        for j in range(CHUNKS):
            for i, dx in enumerate((0, -1, 1, 2)):
                arrived(slot(p, j, dx, 1 - core), s_recv.at[p, j, i])

    def multiply(k, p, lo=0, hi=CHUNKS):
        depth = (hi - lo) * 8 * CROWS
        lhs_t[:, :depth] = jnp.transpose(abuf[k, planes[p], lo:hi].reshape(depth, DROWS))

        def tile(t, carry):
            at = pl.ds(pl.multiple_of(t * TILE, TILE), TILE)
            rhs = bbuf[planes[p], lo:hi, :, :, at].reshape(depth, TILE)
            part = jnp.dot(lhs_t[:, :depth], rhs, preferred_element_type=jnp.float32)
            if p == 0 and lo == 0:
                grad[:, at] = part
            else:
                grad[:, at] += part
            return carry

        lax.fori_loop(0, COLS // TILE, tile, 0, unroll=True)

    bias_one = 1.0 - beta_one**step_count
    bias_two = 1.0 - beta_two**step_count

    def update(k):
        def piece(i, carry):
            r = pl.multiple_of(lax.rem(i, DROWS // 32) * 32, 32)
            at = pl.ds(pl.multiple_of((i // (DROWS // 32)) * TILE, TILE), TILE)
            here = (pl.ds(k * DROWS + r, 32), at)
            g = grad[pl.ds(r, 32), at]
            m1 = beta_one * mom1[here] + (1.0 - beta_one) * g
            m2 = beta_two * mom2[here] + (1.0 - beta_two) * g * g
            w = master[here]
            step = m1 * (1.0 / bias_one) / (jnp.sqrt(m2 * (1.0 / bias_two)) + epsilon)
            w = w - learn_rate * (step + decay_rate * w)
            new_mom1[here] = m1
            new_mom2[here] = m2
            new_master[here] = w
            value[pl.ds(r, 32), at] = w.astype(jnp.bfloat16)
            return carry

        lax.fori_loop(0, (DROWS // 32) * (COLS // TILE), piece, 0, unroll=4)

    lane_fold = lax.broadcasted_iota(jnp.int32, (FOLD, LANES), 1)
    lane_all = lax.broadcasted_iota(jnp.int32, (DROWS, LANES), 1)

    def shifted(val, by):
        by = by % LANES
        return val if by == 0 else pltpu.roll(val, by, 1)

    def pack():
        for u in range(GROUPS):
            at = u * UNIT
            packed[u, :, :UNIT] = value[:PACKED, at : at + UNIT]
            for g in range(PACKED // FOLD):
                extra = value[PACKED:, at + 16 * g : at + 16 * g + 16]
                packed[u, g * FOLD : (g + 1) * FOLD, UNIT:] = extra

    def spread(k):
        def to_slot(i, carry):
            sends[k, i] = packed[index[0, lax.rem(ex + i, GROUPS)]]
            return carry

        lax.fori_loop(0, GROUPS, to_slot, 0)
        for i in (2, 6, 10, 14, 1, 3, 5, 7, 9, 11, 13, 15, 8, 4, 12):
            to = lax.rem(ex + i, GROUPS)
            send(sends.at[k, i], recvs[k].at[ex], e_send.at[k, i], e_recv.at[k, i], (dp, to))
        recvs[k][ex] = sends[k, 0]

    def collect(k):
        for i in range(1, GROUPS):
            arrived(recvs[k].at[lax.rem(ex - i + GROUPS, GROUPS)], e_recv.at[k, i])

        def unfolded(p):
            data = recvs[k][index[1, p]]
            tail = jnp.zeros((FOLD, LANES), data.dtype)
            for g in range(PACKED // FOLD):
                moved = shifted(data[g * FOLD : (g + 1) * FOLD], 16 * g - UNIT)
                tail = jnp.where((lane_fold >= 16 * g) & (lane_fold < 16 * g + 16), moved, tail)
            return jnp.concatenate([data, tail], axis=0)

        held = unfolded(0)
        pos = 0
        for q in range(COLS // LANES):
            off = q * LANES - pos * UNIT
            nxt = unfolded(pos + 1)
            a = shifted(held, -off)
            b = shifted(nxt, UNIT - off)
            joined = jnp.where(lane_all < UNIT - off, a, b)
            out_ref[k * DROWS : (k + 1) * DROWS, q * LANES : (q + 1) * LANES] = joined
            pos += 1
            held = nxt
            if (q + 1) * LANES - pos * UNIT == UNIT and pos + 1 < GROUPS:
                pos += 1
                held = unfolded(pos)

    for j in range(CHUNKS):
        z_out(j)
        center(0, j)
    a_within(0)
    for k in range(PARTS):
        for j in range(CHUNKS):
            abuf[k, plane, j, x * 2 + core] = og[j, :, a_columns(k, dp)]

    for load in loads[8:]:
        load.wait()
    wide = lax.broadcasted_iota(jnp.int32, (GROUPS, 256), 1) // GROUPS
    high = lax.broadcasted_iota(jnp.int32, (GROUPS, 1), 0)
    have = jnp.zeros((GROUPS, 1), jnp.int32)
    wanted = jnp.zeros((GROUPS, 1), jnp.int32)
    for u in range(GROUPS):
        have = jnp.where(high == u, lsm_ref[0, ex * GROUPS + u], have)
        wanted = jnp.where(high == u, rsm_ref[0, ex * GROUPS + u], wanted)
    target = jnp.max(jnp.where(rrow[...] == have, wide, 0), axis=1, keepdims=True)
    source = jnp.max(jnp.where(lrow[...] == wanted, wide, 0), axis=1, keepdims=True)
    low = lax.broadcasted_iota(jnp.int32, (GROUPS, 128), 1)
    high = lax.broadcasted_iota(jnp.int32, (GROUPS, 128), 0)
    index_v[0:1, :] = jnp.max(jnp.where(target == low, high, 0), axis=0, keepdims=True)
    index_v[1:2, :] = jnp.max(jnp.where(high == low, source, 0), axis=0, keepdims=True)
    to_scalar = pltpu.make_async_copy(index_v, index, load_sem.at[10])

    sides(0, 0)
    sides(0, 1)
    to_scalar.start()
    z_in(0)
    sides(0, 2)
    sides(0, 3)
    z_in(1)
    a_across(0)
    opposite(0, 0)
    opposite(0, 1)
    z_in(2)
    opposite(0, 2)
    opposite(0, 3)
    sides(1, 0)
    z_in(3)
    a_across(1)
    a_within(1)
    to_scalar.wait()
    for load in loads[5:8]:
        load.wait()
    sides(1, 1)
    wait_sibling(0)
    wait_a(0, 0)
    multiply(0, 0, 0, 2)
    sides(1, 2)
    multiply(0, 0, 2, 4)
    sides(1, 3)
    for j in range(CHUNKS):
        opposite(1, j)
    wait_sibling(1)
    wait_a(0, 1)
    multiply(0, 1)
    update(0)
    pack()
    spread(0)
    wait_a(1, 0)
    multiply(1, 0)
    wait_a(1, 1)
    multiply(1, 1)
    update(1)
    pack()
    spread(1)
    for copy in started[: 1 - GROUPS]:
        copy.wait_send()
    collect(0)
    for copy in started[1 - GROUPS :]:
        copy.wait_send()
    collect(1)


def step_call(hidden, outgrad, row_expert, counts, learner_map, rollout_map, master, mom1, mom2):
    vmem = pl.BlockSpec(memory_space=pltpu.VMEM)
    hbm = pl.BlockSpec(memory_space=pltpu.HBM)
    dma = pltpu.SemaphoreType.DMA
    state = pltpu.VMEM((WIDTH, COLS), jnp.float32)

    def far(value):
        return pltpu.with_memory_space_constraint(value, pltpu.HBM)

    return pl.pallas_call(
        step_kernel,
        name="grad_update_spread",
        out_shape=(state, state, state, pltpu.VMEM((WIDTH, COLS), jnp.bfloat16)),
        in_specs=[hbm] * 5 + [pl.BlockSpec(memory_space=pltpu.SMEM)] + [hbm] * 3,
        out_specs=(vmem, vmem, vmem, vmem),
        scratch_shapes=[
            pltpu.VMEM((TOK, COLS), jnp.bfloat16),
            pltpu.VMEM((CHUNKS, CROWS, D), jnp.bfloat16),
            pltpu.VMEM((1, TOK), jnp.int32),
            pltpu.VMEM((1, 256), jnp.int32),
            pltpu.VMEM((1, 256), jnp.int32),
            pltpu.SMEM((1, 256), jnp.int32),
            pltpu.SMEM((1, 256), jnp.int32),
            pltpu.VMEM((WIDTH, COLS), jnp.float32),
            pltpu.VMEM((WIDTH, COLS), jnp.float32),
            pltpu.VMEM((WIDTH, COLS), jnp.float32),
            pltpu.VMEM((PARTS, 2, CHUNKS, 8, CROWS, DROWS), jnp.bfloat16),
            pltpu.VMEM((2, CHUNKS, 8, CROWS, COLS), jnp.bfloat16),
            pltpu.VMEM((DROWS, 8 * TOK), jnp.bfloat16),
            pltpu.VMEM((DROWS, COLS), jnp.float32),
            pltpu.VMEM((2, 128), jnp.int32),
            pltpu.SMEM((2, 128), jnp.int32),
            pltpu.VMEM((DROWS, COLS), jnp.bfloat16),
            pltpu.VMEM((GROUPS, PACKED, LANES), jnp.bfloat16),
            pltpu.VMEM((PARTS, GROUPS, PACKED, LANES), jnp.bfloat16),
            pltpu.VMEM((GROUPS, PACKED, LANES), jnp.bfloat16),
            pltpu.VMEM((GROUPS, PACKED, LANES), jnp.bfloat16),
            dma((11,)),
            dma((PARTS, 16)), dma((PARTS, 16)),
            dma((CHUNKS,)), dma((CHUNKS,)),
            dma((2, CHUNKS, 2)), dma((2, CHUNKS, 2)),
            dma((2, CHUNKS, 2)), dma((2, CHUNKS, 2)),
            dma((2, CHUNKS, 4)), dma((2, CHUNKS, 4)),
            dma((PARTS, GROUPS)), dma((PARTS, GROUPS)),
        ],
        compiler_params=pltpu.CompilerParams(
            collective_id=0, has_side_effects=True, vmem_limit_bytes=40 * 1024 * 1024
        ),
    )(
        far(hidden),
        far(outgrad.reshape(CHUNKS, CROWS, D)),
        far(row_expert),
        far(learner_map.reshape(1, 256)),
        far(rollout_map.reshape(1, 256)),
        counts,
        far(master),
        far(mom1),
        far(mom2),
    )


def land_kernel(*refs):
    ins, outs, sem = refs[:4], refs[4:8], refs[8]
    copies = [pltpu.make_async_copy(a, b, sem.at[i]) for i, (a, b) in enumerate(zip(ins, outs))]
    for copy in copies:
        copy.start()
    for copy in copies:
        copy.wait()


def land_call(values):
    return pl.pallas_call(
        land_kernel,
        name="land_outputs",
        out_shape=tuple(jax.ShapeDtypeStruct(v.shape, v.dtype) for v in values),
        in_specs=[pl.BlockSpec(memory_space=pltpu.VMEM)] * 4,
        out_specs=(pl.BlockSpec(memory_space=pltpu.HBM),) * 4,
        scratch_shapes=[pltpu.SemaphoreType.DMA((4,))],
        compiler_params=pltpu.CompilerParams(vmem_limit_bytes=4 * 1024 * 1024),
    )(*values)


def on_device(
    hidden, outgrad, row_expert, counts, learner_map, rollout_map, master, moment1, moment2
):
    return land_call(
        step_call(
            hidden[0], outgrad[0], row_expert, counts, learner_map, rollout_map,
            master, moment1, moment2,
        )
    )


def solution(mesh):
    return jax.shard_map(
        on_device,
        mesh=mesh,
        in_specs=(
            P("expert", "dp", None),
            P("expert", "dp", None),
            P("expert", "dp"),
            P("expert", "dp"),
            P(),
            P(),
            P("dp", "expert"),
            P("dp", "expert"),
            P("dp", "expert"),
        ),
        out_specs=(P("dp", "expert"),) * 4,
        check_vma=False,
    )
```

```python
import jax
import jax.numpy as jnp
from jax import lax
from jax.experimental import pallas as pl
from jax.experimental.pallas import tpu as pltpu
from jax.sharding import PartitionSpec as P

MESH = pl.DeviceIdType.MESH
FF = 14336
D = 4096
COLS = 1792
UNIT = 112
GROUPS = 16
HALF_UNITS = FF // UNIT
TOK = 128
CHUNKS = 4
CROWS = TOK // CHUNKS
WIDTH = 256
TILE = 256
PARTS = 2
DROWS = WIDTH // PARTS
FOLD = 16
PACKED = DROWS - FOLD
LANES = 128

beta_one = 0.9
beta_two = 0.95
learn_rate = 0.01
decay_rate = 0.1
epsilon = 1e-08
step_count = 100.0


def dp_of(x, plane, core):
    return (lax.rem(x + 4, 4) * 2 + plane) * 2 + core


def step_kernel(
    hid_ref, og_ref, rexp_ref, lrow_ref, rrow_ref, count_ref,
    master_ref, mom1_ref, mom2_ref,
    new_master, new_mom1, new_mom2, out_ref,
    hid, og, rexp, lrow, rrow, lsm_ref, rsm_ref, master, mom1, mom2, abuf, bbuf, lhs_t, grad,
    index_v, index, value, packed, sends, recv_0, recv_1,
    load_sem, a_send, a_recv, z_send, z_recv, x_send, x_recv, o_send, o_recv, s_send, s_recv,
    e_send, e_recv,
):
    recvs = (recv_0, recv_1)
    dp = lax.axis_index("dp")
    ex = lax.axis_index("expert")
    core = lax.rem(dp, 2)
    plane = lax.rem(dp // 2, 2)
    x = dp // 4
    planes = (plane, 1 - plane)

    barrier = pltpu.get_barrier_semaphore()
    for k in range(1, 16):
        pl.semaphore_signal(barrier, inc=1, device_id=(lax.rem(dp + k, 16), ex), device_id_type=MESH)
    for k in range(1, 16):
        pl.semaphore_signal(barrier, inc=1, device_id=(dp, lax.rem(ex + k, 16)), device_id_type=MESH)
    loads = [
        pltpu.make_async_copy(src, dst, load_sem.at[i])
        for i, (src, dst) in enumerate(
            (
                (lrow_ref, lsm_ref), (rrow_ref, rsm_ref), (hid_ref, hid), (rexp_ref, rexp), (og_ref, og),
                (mom1_ref, mom1), (mom2_ref, mom2), (master_ref, master),
                (lrow_ref, lrow), (rrow_ref, rrow),
            )
        )
    ]
    for load in loads:
        load.start()

    for load in loads[:2]:
        load.wait()
    lane = lax.broadcasted_iota(jnp.int32, (8, COLS), 1)
    unit_of = jnp.zeros((8, COLS), jnp.int32)
    for u in range(GROUPS):
        belongs = (lane >= u * UNIT) & (lane < (u + 1) * UNIT)
        unit_of = jnp.where(belongs, lsm_ref[0, ex * GROUPS + u], unit_of)
    expert_of = jnp.where(unit_of >= HALF_UNITS, 1, 0)[0:1, :]
    rows = lax.broadcasted_iota(jnp.int32, (TOK, TOK), 0)
    cols = lax.broadcasted_iota(jnp.int32, (TOK, TOK), 1)
    for load in loads[2:4]:
        load.wait()
    row_expert = jnp.sum(jnp.where(rows == cols, rexp[...], 0), axis=1, keepdims=True)
    live = lax.broadcasted_iota(jnp.int32, (TOK, 1), 0) < count_ref[0, 0]
    row_key = jnp.where(live, row_expert, -1)
    for j in range(CHUNKS):
        key = row_key[j * CROWS : (j + 1) * CROWS]
        kept = key == expert_of
        block = hid[j * CROWS : (j + 1) * CROWS, :].astype(jnp.float32)
        bbuf[plane, j, x * 2 + core] = jnp.where(kept, block, 0.0).astype(jnp.bfloat16)
    loads[4].wait()
    pl.semaphore_wait(barrier, 30)

    started = []

    def send(src, dst, ssem, rsem, to):
        copy = pltpu.make_async_remote_copy(
            src_ref=src, dst_ref=dst, send_sem=ssem, recv_sem=rsem,
            device_id=to, device_id_type=MESH,
        )
        copy.start()
        started.append(copy)

    def arrived(ref, rsem):
        pltpu.make_async_copy(ref, ref, rsem).wait()

    def a_columns(k, other):
        return pl.ds(pl.multiple_of(other * WIDTH + k * DROWS, DROWS), DROWS)

    def send_a(k, other):
        cut = og.at[:, :, a_columns(k, other)]
        slot_a = abuf.at[k, plane, :, x * 2 + core]
        send(cut, slot_a, a_send.at[k, other], a_recv.at[k, dp], (other, ex))

    def a_across(k):
        for dx in (0, 1, 3, 2):
            for dc in range(2):
                send_a(k, dp_of(x + dx, 1 - plane, lax.rem(core + dc, 2)))

    def a_within(k):
        for dx in (1, 3, 2, 0):
            for dc in range(2):
                if (dx, dc) != (0, 0):
                    send_a(k, dp_of(x + dx, plane, lax.rem(core + dc, 2)))

    def slot(p, j, dx, c):
        return bbuf.at[planes[p], j, lax.rem(x + dx + 4, 4) * 2 + c]

    def peer(dx, c):
        return (dp_of(x + dx, plane, c), ex)

    def center(p, j):
        me = slot(p, j, 0, core)
        send(me, me, x_send.at[p, j, 0], x_recv.at[p, j, 0], peer(1, core))
        send(me, me, x_send.at[p, j, 1], x_recv.at[p, j, 1], peer(-1, core))
        send(me, me, s_send.at[p, j, 0], s_recv.at[p, j, 0], peer(0, 1 - core))

    def z_out(j):
        me = slot(0, j, 0, core)
        send(me, me, z_send.at[j], z_recv.at[j], (dp_of(x, 1 - plane, core), ex))

    def z_in(j):
        arrived(slot(1, j, 0, core), z_recv.at[j])
        center(1, j)

    def sides(p, j):
        left = slot(p, j, -1, core)
        arrived(left, x_recv.at[p, j, 0])
        first = left.at[pl.ds(0, CROWS // 2)]
        send(first, first, o_send.at[p, j, 0], o_recv.at[p, j, 0], peer(1, core))
        send(left, left, s_send.at[p, j, 1], s_recv.at[p, j, 1], peer(0, 1 - core))
        right = slot(p, j, 1, core)
        arrived(right, x_recv.at[p, j, 1])
        second = right.at[pl.ds(CROWS // 2, CROWS // 2)]
        send(second, second, o_send.at[p, j, 1], o_recv.at[p, j, 1], peer(-1, core))
        send(right, right, s_send.at[p, j, 2], s_recv.at[p, j, 2], peer(0, 1 - core))

    def opposite(p, j):
        far = slot(p, j, 2, core)
        arrived(far.at[pl.ds(0, CROWS // 2)], o_recv.at[p, j, 0])
        arrived(far.at[pl.ds(CROWS // 2, CROWS // 2)], o_recv.at[p, j, 1])
        send(far, far, s_send.at[p, j, 3], s_recv.at[p, j, 3], peer(0, 1 - core))

    def wait_a(k, p):
        for dx in range(4):
            for dc in range(2):
                if (p, dx, dc) == (0, 0, 0):
                    continue
                c = lax.rem(core + dc, 2)
                src = dp_of(x + dx, planes[p], c)
                arrived(abuf.at[k, planes[p], :, lax.rem(x + dx, 4) * 2 + c], a_recv.at[k, src])

    def wait_sibling(p):
        for j in range(CHUNKS):
            for i, dx in enumerate((0, -1, 1, 2)):
                arrived(slot(p, j, dx, 1 - core), s_recv.at[p, j, i])

    def multiply(k, p, lo=0, hi=CHUNKS):
        depth = (hi - lo) * 8 * CROWS
        lhs_t[:, :depth] = jnp.transpose(abuf[k, planes[p], lo:hi].reshape(depth, DROWS))

        def tile(t, carry):
            at = pl.ds(pl.multiple_of(t * TILE, TILE), TILE)
            rhs = bbuf[planes[p], lo:hi, :, :, at].reshape(depth, TILE)
            part = jnp.dot(lhs_t[:, :depth], rhs, preferred_element_type=jnp.float32)
            if p == 0 and lo == 0:
                grad[:, at] = part
            else:
                grad[:, at] += part
            return carry

        lax.fori_loop(0, COLS // TILE, tile, 0, unroll=True)

    bias_one = 1.0 - beta_one**step_count
    bias_two = 1.0 - beta_two**step_count

    def update(k):
        def piece(i, carry):
            r = pl.multiple_of(lax.rem(i, DROWS // 32) * 32, 32)
            at = pl.ds(pl.multiple_of((i // (DROWS // 32)) * TILE, TILE), TILE)
            here = (pl.ds(k * DROWS + r, 32), at)
            g = grad[pl.ds(r, 32), at]
            m1 = beta_one * mom1[here] + (1.0 - beta_one) * g
            m2 = beta_two * mom2[here] + (1.0 - beta_two) * g * g
            w = master[here]
            step = m1 * (1.0 / bias_one) / (jnp.sqrt(m2 * (1.0 / bias_two)) + epsilon)
            w = w - learn_rate * (step + decay_rate * w)
            new_mom1[here] = m1
            new_mom2[here] = m2
            new_master[here] = w
            value[pl.ds(r, 32), at] = w.astype(jnp.bfloat16)
            return carry

        lax.fori_loop(0, (DROWS // 32) * (COLS // TILE), piece, 0, unroll=7)

    lane_fold = lax.broadcasted_iota(jnp.int32, (FOLD, LANES), 1)
    lane_all = lax.broadcasted_iota(jnp.int32, (DROWS, LANES), 1)

    def shifted(val, by):
        by = by % LANES
        return val if by == 0 else pltpu.roll(val, by, 1)

    def pack():
        for u in range(GROUPS):
            at = u * UNIT
            packed[u, :, :UNIT] = value[:PACKED, at : at + UNIT]
            for g in range(PACKED // FOLD):
                extra = value[PACKED:, at + 16 * g : at + 16 * g + 16]
                packed[u, g * FOLD : (g + 1) * FOLD, UNIT:] = extra

    def spread(k):
        def to_slot(i, carry):
            sends[k, i] = packed[index[0, lax.rem(ex + i, GROUPS)]]
            return carry

        lax.fori_loop(0, GROUPS, to_slot, 0)
        for i in (2, 6, 10, 14, 1, 3, 5, 7, 9, 11, 13, 15, 8, 4, 12):
            to = lax.rem(ex + i, GROUPS)
            send(sends.at[k, i], recvs[k].at[ex], e_send.at[k, i], e_recv.at[k, i], (dp, to))
        recvs[k][ex] = sends[k, 0]

    def collect(k):
        for i in range(1, GROUPS):
            arrived(recvs[k].at[lax.rem(ex - i + GROUPS, GROUPS)], e_recv.at[k, i])

        def unfolded(p):
            data = recvs[k][index[1, p]]
            tail = jnp.zeros((FOLD, LANES), data.dtype)
            for g in range(PACKED // FOLD):
                moved = shifted(data[g * FOLD : (g + 1) * FOLD], 16 * g - UNIT)
                tail = jnp.where((lane_fold >= 16 * g) & (lane_fold < 16 * g + 16), moved, tail)
            return jnp.concatenate([data, tail], axis=0)

        held = unfolded(0)
        pos = 0
        for q in range(COLS // LANES):
            off = q * LANES - pos * UNIT
            nxt = unfolded(pos + 1)
            a = shifted(held, -off)
            b = shifted(nxt, UNIT - off)
            joined = jnp.where(lane_all < UNIT - off, a, b)
            out_ref[k * DROWS : (k + 1) * DROWS, q * LANES : (q + 1) * LANES] = joined
            pos += 1
            held = nxt
            if (q + 1) * LANES - pos * UNIT == UNIT and pos + 1 < GROUPS:
                pos += 1
                held = unfolded(pos)

    for j in range(CHUNKS):
        z_out(j)
        center(0, j)
    a_within(0)
    for k in range(PARTS):
        for j in range(CHUNKS):
            abuf[k, plane, j, x * 2 + core] = og[j, :, a_columns(k, dp)]

    for load in loads[8:]:
        load.wait()
    wide = lax.broadcasted_iota(jnp.int32, (GROUPS, 256), 1) // GROUPS
    high = lax.broadcasted_iota(jnp.int32, (GROUPS, 1), 0)
    have = jnp.zeros((GROUPS, 1), jnp.int32)
    wanted = jnp.zeros((GROUPS, 1), jnp.int32)
    for u in range(GROUPS):
        have = jnp.where(high == u, lsm_ref[0, ex * GROUPS + u], have)
        wanted = jnp.where(high == u, rsm_ref[0, ex * GROUPS + u], wanted)
    target = jnp.max(jnp.where(rrow[...] == have, wide, 0), axis=1, keepdims=True)
    source = jnp.max(jnp.where(lrow[...] == wanted, wide, 0), axis=1, keepdims=True)
    low = lax.broadcasted_iota(jnp.int32, (GROUPS, 128), 1)
    high = lax.broadcasted_iota(jnp.int32, (GROUPS, 128), 0)
    index_v[0:1, :] = jnp.max(jnp.where(target == low, high, 0), axis=0, keepdims=True)
    index_v[1:2, :] = jnp.max(jnp.where(high == low, source, 0), axis=0, keepdims=True)
    to_scalar = pltpu.make_async_copy(index_v, index, load_sem.at[10])

    sides(0, 0)
    sides(0, 1)
    to_scalar.start()
    z_in(0)
    sides(0, 2)
    sides(0, 3)
    z_in(1)
    a_across(0)
    opposite(0, 0)
    opposite(0, 1)
    z_in(2)
    opposite(0, 2)
    opposite(0, 3)
    sides(1, 0)
    z_in(3)
    a_across(1)
    a_within(1)
    to_scalar.wait()
    for load in loads[5:8]:
        load.wait()
    sides(1, 1)
    wait_sibling(0)
    wait_a(0, 0)
    multiply(0, 0, 0, 2)
    sides(1, 2)
    multiply(0, 0, 2, 4)
    sides(1, 3)
    for j in range(CHUNKS):
        opposite(1, j)
    wait_sibling(1)
    wait_a(0, 1)
    multiply(0, 1)
    update(0)
    pack()
    spread(0)
    wait_a(1, 0)
    multiply(1, 0)
    wait_a(1, 1)
    multiply(1, 1)
    update(1)
    pack()
    spread(1)
    for copy in started[: 1 - GROUPS]:
        copy.wait_send()
    collect(0)
    for copy in started[1 - GROUPS :]:
        copy.wait_send()
    collect(1)


def step_call(hidden, outgrad, row_expert, counts, learner_map, rollout_map, master, mom1, mom2):
    vmem = pl.BlockSpec(memory_space=pltpu.VMEM)
    hbm = pl.BlockSpec(memory_space=pltpu.HBM)
    dma = pltpu.SemaphoreType.DMA
    state = pltpu.VMEM((WIDTH, COLS), jnp.float32)

    def far(value):
        return pltpu.with_memory_space_constraint(value, pltpu.HBM)

    return pl.pallas_call(
        step_kernel,
        name="grad_update_spread",
        out_shape=(state, state, state, pltpu.VMEM((WIDTH, COLS), jnp.bfloat16)),
        in_specs=[hbm] * 5 + [pl.BlockSpec(memory_space=pltpu.SMEM)] + [hbm] * 3,
        out_specs=(vmem, vmem, vmem, vmem),
        scratch_shapes=[
            pltpu.VMEM((TOK, COLS), jnp.bfloat16),
            pltpu.VMEM((CHUNKS, CROWS, D), jnp.bfloat16),
            pltpu.VMEM((1, TOK), jnp.int32),
            pltpu.VMEM((1, 256), jnp.int32),
            pltpu.VMEM((1, 256), jnp.int32),
            pltpu.SMEM((1, 256), jnp.int32),
            pltpu.SMEM((1, 256), jnp.int32),
            pltpu.VMEM((WIDTH, COLS), jnp.float32),
            pltpu.VMEM((WIDTH, COLS), jnp.float32),
            pltpu.VMEM((WIDTH, COLS), jnp.float32),
            pltpu.VMEM((PARTS, 2, CHUNKS, 8, CROWS, DROWS), jnp.bfloat16),
            pltpu.VMEM((2, CHUNKS, 8, CROWS, COLS), jnp.bfloat16),
            pltpu.VMEM((DROWS, 8 * TOK), jnp.bfloat16),
            pltpu.VMEM((DROWS, COLS), jnp.float32),
            pltpu.VMEM((2, 128), jnp.int32),
            pltpu.SMEM((2, 128), jnp.int32),
            pltpu.VMEM((DROWS, COLS), jnp.bfloat16),
            pltpu.VMEM((GROUPS, PACKED, LANES), jnp.bfloat16),
            pltpu.VMEM((PARTS, GROUPS, PACKED, LANES), jnp.bfloat16),
            pltpu.VMEM((GROUPS, PACKED, LANES), jnp.bfloat16),
            pltpu.VMEM((GROUPS, PACKED, LANES), jnp.bfloat16),
            dma((11,)),
            dma((PARTS, 16)), dma((PARTS, 16)),
            dma((CHUNKS,)), dma((CHUNKS,)),
            dma((2, CHUNKS, 2)), dma((2, CHUNKS, 2)),
            dma((2, CHUNKS, 2)), dma((2, CHUNKS, 2)),
            dma((2, CHUNKS, 4)), dma((2, CHUNKS, 4)),
            dma((PARTS, GROUPS)), dma((PARTS, GROUPS)),
        ],
        compiler_params=pltpu.CompilerParams(
            collective_id=0, has_side_effects=True, vmem_limit_bytes=40 * 1024 * 1024
        ),
    )(
        far(hidden),
        far(outgrad.reshape(CHUNKS, CROWS, D)),
        far(row_expert),
        far(learner_map.reshape(1, 256)),
        far(rollout_map.reshape(1, 256)),
        counts,
        far(master),
        far(mom1),
        far(mom2),
    )


def land_kernel(*refs):
    ins, outs, sem = refs[:4], refs[4:8], refs[8]
    copies = [pltpu.make_async_copy(a, b, sem.at[i]) for i, (a, b) in enumerate(zip(ins, outs))]
    for copy in copies:
        copy.start()
    for copy in copies:
        copy.wait()


def land_call(values):
    return pl.pallas_call(
        land_kernel,
        name="land_outputs",
        out_shape=tuple(jax.ShapeDtypeStruct(v.shape, v.dtype) for v in values),
        in_specs=[pl.BlockSpec(memory_space=pltpu.VMEM)] * 4,
        out_specs=(pl.BlockSpec(memory_space=pltpu.HBM),) * 4,
        scratch_shapes=[pltpu.SemaphoreType.DMA((4,))],
        compiler_params=pltpu.CompilerParams(vmem_limit_bytes=4 * 1024 * 1024),
    )(*values)


def on_device(
    hidden, outgrad, row_expert, counts, learner_map, rollout_map, master, moment1, moment2
):
    return land_call(
        step_call(
            hidden[0], outgrad[0], row_expert, counts, learner_map, rollout_map,
            master, moment1, moment2,
        )
    )


def solution(mesh):
    return jax.shard_map(
        on_device,
        mesh=mesh,
        in_specs=(
            P("expert", "dp", None),
            P("expert", "dp", None),
            P("expert", "dp"),
            P("expert", "dp"),
            P(),
            P(),
            P("dp", "expert"),
            P("dp", "expert"),
            P("dp", "expert"),
        ),
        out_specs=(P("dp", "expert"),) * 4,
        check_vma=False,
    )
```
